32 devices in a mesh: rep: 2 (over x), shard: 16 (over z, y, core).
Axes of the slice: x: 2, y: 2, z: 4, core: 2. Of those that a mesh axis runs over, the one named last changes fastest.
Arguments:
- dense: bfloat16 [8192, 128], P(('rep', 'shard')), may hold values from -6 to 6
- small_ids: int32 [8192, 32], P(('rep', 'shard')), may hold values from 0 to 511
- labels: int32 [8192], P(('rep', 'shard')), may hold values 0 or 1
- small_tables: bfloat16 [32, 512, 128], replicated, may hold values from -6 to 6
- large_tables: bfloat16 [16, 8192, 128], P('shard'), may hold values from -6 to 6
- batch_sizes: int32 [16, 32], replicated, may hold values from 1 to 128, as said below
- bag_ends: int32 [16, 32, 128], P('shard'), may hold values from 0 to 256, as said below
- owner_row_index: int32 [16, 32, 256], P('shard'), may hold values from 0 to 8191
- w_first: bfloat16 [1304, 1024], replicated, may hold values from -0.15625 to 0.15625
- b_first: float32 [1024], replicated, may hold values from -3 to 3
- w_out: float32 [1024], replicated, may hold values from -0.1875 to 0.1875
Outputs:
- small_new: bfloat16 [32, 512, 128], replicated
- large_new: bfloat16 [16, 8192, 128], P('shard')
The draws below stay inside these ranges and needn't reach their ends.
Inputs may be any that keep to these rules, and one draw needn't show every extreme that they name: `batch_sizes`: every feature has some owner, and every owner some feature, with exactly 128. `bag_ends`: nondecreasing along the last dimension; bags j >= batch_sizes[f, d] are empty; some bag list reaches 256.
All inputs are finite; a program needn't handle non-finite values. No bound on the sum of `labels` on one device may be relied on, other than what follows from the above.
Results may differ from the reference program's by a relative error of at most 0.0095.
Values may be sent and summed in bfloat16 or wider, within the bound.
A program may use at most 192 MiB of HBM per device.

```python
import math
import jax
import jax.numpy as jnp
import numpy as np
from jax import lax

E = 128
SROWS = 512
NSMALL = 32
LROWS = 8192
HID1 = 1024
PMAX = 3
BATCH = 256
BSMAX = 128
SLOTS = 256
FEAT = 16
DEST = 32
ROWS = 8192
PAIRS = 1176


def batch_table(key):
    folded = jax.random.fold_in(key, 7301)
    first_key, second_key, third_key = jax.random.split(folded, 3)
    size_table = jax.random.randint(first_key, (FEAT, DEST), 1, BSMAX + 1)
    pick_feature = jax.random.randint(second_key, (DEST,), 0, FEAT)
    pick_owner = jax.random.randint(third_key, (FEAT,), 0, DEST)
    forced = (jnp.arange(FEAT)[:, None] == pick_feature[None, :]) | (jnp.arange(DEST)[None, :] == pick_owner[:, None])
    return jnp.where(forced, BSMAX, size_table).astype(jnp.int32)


def draw_batch_sizes(key, part):
    return batch_table(key)


def draw_bag_ends(key, part):
    size_table = batch_table(key)
    lengths = jax.random.randint(jax.random.fold_in(key, 7302), (FEAT, DEST, BSMAX), 1, PMAX + 1)
    lengths = jnp.where(size_table[:, :, None] == BSMAX, PMAX, lengths)
    active = jnp.arange(BSMAX)[None, None, :] < size_table[:, :, None]
    limits = jnp.cumsum(jnp.where(active, lengths, 0), axis=2)
    return jnp.minimum(limits, SLOTS).astype(jnp.int32)


def touch_ends(result, stream_key, smallest, top_value):
    place = [jax.random.randint(jax.random.fold_in(stream_key, axis), (), 0, length) for axis, length in enumerate(result.shape)]
    widest = result.shape.index(max(result.shape))
    neighbour = place[:widest] + [(place[widest] + 1) % result.shape[widest]] + place[widest + 1:]
    return result.at[tuple(place)].set(smallest).at[tuple(neighbour)].set(top_value)


def block_levels(own_key, dims, cuts, least, largest):
    gain, own = 1.0, jax.random.fold_in(own_key, 6)
    for position, blocks in cuts:
        heights = jnp.exp(jax.random.uniform(jax.random.fold_in(own, position), (blocks,), jnp.float32, least / len(cuts), largest / len(cuts)))
        gain = gain * jnp.repeat(heights, dims[position] // blocks).reshape([-1 if axis == position else 1 for axis in range(len(dims))])
    return gain


def rank_table(amount, lean):
    weights = [(1 << 20) // math.isqrt(standing ** lean) + 1 for standing in range(1, amount + 1)]
    deviation = 1 + sum(weights) // (1 << 30)
    return np.cumsum(np.array([max(1, weight // deviation) for weight in weights]))


def skewed_ids(own_key, shape, amount, lean):
    grid = rank_table(amount, lean)
    ticket = jax.random.randint(jax.random.fold_in(own_key, 1), shape, 0, int(grid[amount - 1]))
    grade = jnp.searchsorted(jnp.asarray(grid, jnp.int32), ticket, side="right")
    return jax.random.permutation(jax.random.fold_in(own_key, 2), amount)[grade].astype(jnp.int32)


def normal_values(rng, shape, spread, bound, shards=(), held_as=jnp.bfloat16):
    entries = jax.random.normal(rng, shape, jnp.float32) * spread
    if len(shards) > 0:
        entries = block_levels(rng, shape, shards, -0.22, 0.18) * entries
    return jnp.clip(entries, min=-bound, max=bound).astype(held_as)


def setup_inputs(seed: int = 0) -> dict:
    splits = jax.random.split(jax.random.key(seed), 12)
    return {
        "dense": normal_values(splits[0], (ROWS, E), 1.0, 6.0, ((0, 32),)),
        "small_ids": touch_ends(jax.random.randint(splits[1], (ROWS, NSMALL), 0, SROWS), jax.random.fold_in(splits[1], 1), 0, SROWS - 1).astype(jnp.int32),
        "labels": touch_ends((jax.random.randint(splits[2], (ROWS,), 0, 4) < 1).astype(jnp.int32), jax.random.fold_in(splits[2], 1), 0, 1),
        "small_tables": normal_values(splits[3], (NSMALL, SROWS, E), 1.0, 6.0),
        "large_tables": normal_values(splits[4], (FEAT, LROWS, E), 1.0, 6.0, ((0, 16),)),
        "batch_sizes": draw_batch_sizes(jax.random.fold_in(splits[11], 71), 0),
        "bag_ends": draw_bag_ends(jax.random.fold_in(splits[11], 71), 0),
        "owner_row_index": touch_ends(skewed_ids(splits[7], (FEAT, DEST, SLOTS), LROWS, 2), jax.random.fold_in(splits[7], 3), 0, LROWS - 1).astype(jnp.int32),
        "w_first": normal_values(splits[8], (PAIRS + E, HID1), (PAIRS + E) ** -0.5, 0.15625),
        "b_first": normal_values(splits[9], (HID1,), 0.5, 3.0, (), jnp.float32),
        "w_out": normal_values(splits[10], (HID1,), HID1 ** -0.5, 0.1875, (), jnp.float32),
    }


step_size = 32.0

def bag_members(limits):
    starts = jnp.concatenate([jnp.zeros(limits.shape[:-1] + (1,), jnp.int32), limits[..., :-1]], axis=-1)
    positions = jnp.arange(SLOTS, dtype=jnp.int32)
    inside = (positions >= starts[..., None]) & (positions < limits[..., None])
    return inside.astype(jnp.float32)

def silu_slope(preacts):
    squash = jax.nn.sigmoid(preacts)
    return squash * (1.0 + preacts * (1.0 - squash))

def reference(dense, small_ids, labels, small_tables, large_tables, batch_sizes, bag_ends, owner_row_index, w_first, b_first, w_out):
    vec_count = 1 + NSMALL + FEAT
    lower_rows, lower_cols = np.tril_indices(vec_count, -1)

    def pool_one(packed):
        table_one, row_list, limits = packed
        bag_entry = bag_members(limits)
        collected_rows = table_one[row_list].astype(jnp.float32)
        return jnp.einsum('hxt,htv->hxv', bag_entry, collected_rows).astype(jnp.bfloat16)
    pooled = lax.map(pool_one, (large_tables, owner_row_index, bag_ends))
    pooled_dev = jnp.moveaxis(pooled, 1, 0)
    dense_blocks = dense.reshape(DEST, BATCH, E)
    id_blocks = small_ids.reshape(DEST, BATCH, NSMALL)
    label_blocks = labels.reshape(DEST, BATCH).astype(jnp.float32)
    size_blocks = jnp.transpose(batch_sizes)
    samples = jnp.arange(BATCH, dtype=jnp.int32)
    table_offsets = jnp.arange(NSMALL, dtype=jnp.int32) * SROWS
    feat_offsets = jnp.arange(FEAT, dtype=jnp.int32) * BSMAX

    def device_step(totals, inputs):
        dense_b, ids_b, label_b, pooled_b, size_row = inputs
        chosen = samples[None, :] * size_row[:, None] // BATCH
        large_feat = jnp.take_along_axis(pooled_b, chosen[:, :, None].astype(jnp.int32), axis=1)
        large_feat = jnp.transpose(large_feat, (1, 0, 2))
        minor_feature = small_tables[jnp.arange(NSMALL)[None, :], ids_b]
        vectors = jnp.concatenate([dense_b[:, None, :], minor_feature, large_feat], axis=1)
        vec_float = vectors.astype(jnp.float32)
        gram_matrix = jnp.einsum('bie,bje->bij', vec_float, vec_float)
        pair_values = (gram_matrix[:, lower_rows, lower_cols] * E ** (-0.5)).astype(jnp.bfloat16)
        features = jnp.concatenate([pair_values, dense_b], axis=1)
        preact = jnp.dot(features, w_first, preferred_element_type=jnp.float32) + b_first
        hidden = jax.nn.silu(preact)
        logits = lax.optimization_barrier(jnp.sum(hidden * w_out[None, :], axis=1))
        logit_grad = jax.nn.sigmoid(logits) - label_b
        pre_grad = (logit_grad[:, None] * w_out[None, :] * silu_slope(preact)).astype(jnp.bfloat16)
        pair_grad = jnp.dot(pre_grad, jnp.transpose(w_first[:PAIRS]), preferred_element_type=jnp.float32) * E ** (-0.5)
        lower_part = jnp.zeros((BATCH, vec_count, vec_count), jnp.float32).at[:, lower_rows, lower_cols].set(pair_grad)
        vec_grad = jnp.einsum('bij,bje->bie', lower_part + jnp.swapaxes(lower_part, 1, 2), vec_float).astype(jnp.bfloat16)
        small_part = vec_grad[:, 1:1 + NSMALL].astype(jnp.float32).reshape(-1, E)
        small_index = (table_offsets[None, :] + ids_b).reshape(-1).astype(jnp.int32)
        totals = totals + jax.ops.segment_sum(small_part, small_index, NSMALL * SROWS)
        large_part = jnp.transpose(vec_grad[:, 1 + NSMALL:], (1, 0, 2)).astype(jnp.float32).reshape(-1, E)
        large_index = (feat_offsets[:, None] + chosen).reshape(-1).astype(jnp.int32)
        accumulate_gradient = jax.ops.segment_sum(large_part, large_index, FEAT * BSMAX).reshape(FEAT, BSMAX, E).astype(jnp.bfloat16)
        return (totals, accumulate_gradient)
    start_totals = jnp.zeros((NSMALL * SROWS, E), jnp.float32)
    small_grad, fold_all = lax.scan(device_step, start_totals, (dense_blocks, id_blocks, label_blocks, pooled_dev, size_blocks))
    fold_feat = jnp.moveaxis(fold_all, 0, 1)

    def table_grad(packed):
        row_list, limits, gradient_list = packed
        bag_entry = bag_members(limits)
        slot_vectors = jnp.einsum('bni,bnv->biv', bag_entry, gradient_list.astype(jnp.float32))
        return jax.ops.segment_sum(slot_vectors.reshape(-1, E), row_list.reshape(-1).astype(jnp.int32), LROWS)
    large_grad = lax.map(table_grad, (owner_row_index, bag_ends, fold_feat))
    small_new = (small_tables.astype(jnp.float32) - step_size * small_grad.reshape(NSMALL, SROWS, E)).astype(jnp.bfloat16)
    large_new = (large_tables.astype(jnp.float32) - step_size * large_grad).astype(jnp.bfloat16)
    return (small_new, large_new)
```

```python
import functools

import jax
import jax.numpy as jnp
from jax import lax
from jax.experimental import pallas as pl
from jax.experimental.pallas import tpu as pltpu
from jax.sharding import PartitionSpec as P

step_size = 32.0
LANES = 128
VMEM_LIMIT = 60 * 1024 * 1024
f32 = jnp.float32
bf16 = jnp.bfloat16


def whole(space):
    return pl.BlockSpec(memory_space=space)


def iota(shape, axis):
    return lax.broadcasted_iota(jnp.int32, shape, axis)


def members_of(ends, slots):
    span = ends.shape[-1]
    starts = jnp.where(iota((1, span), 1) == 0, 0, pltpu.roll(ends, 1, 1))
    places = iota((slots, span), 0)
    return ((places >= starts) & (places < ends)).astype(f32).astype(bf16)


def pool_kernel(rows_ref, count_ref, ends_ref, table_ref, out_ref, wide, picked):
    owners, slots = rows_ref.shape
    wide[...] = table_ref[...].astype(f32)
    picked[...] = jnp.zeros_like(picked)

    def owner(d, carry):
        def group(g, c):
            base = pl.multiple_of(g * 8, 8)
            parts = [wide[pl.ds(rows_ref[d, base + u], 1), :] for u in range(8)]
            picked[pl.ds(base, 8), :] = jnp.concatenate(parts, axis=0)
            return c

        lax.fori_loop(0, (count_ref[d] + 7) // 8, group, 0)
        members = members_of(ends_ref[pl.ds(d, 1), :], slots)
        pooled = lax.dot_general(
            members, picked[...].astype(bf16), (((0,), (0,)), ((), ())),
            preferred_element_type=f32,
        )
        out_ref[d] = pooled.astype(bf16)
        return carry

    lax.fori_loop(0, owners, owner, 0)


def pool(rows, counts, ends, table):
    owners, slots = rows.shape
    width = table.shape[1]
    return pl.pallas_call(
        pool_kernel,
        out_shape=jax.ShapeDtypeStruct((owners, ends.shape[1], width), bf16),
        in_specs=[whole(pltpu.SMEM), whole(pltpu.SMEM), whole(pltpu.VMEM), whole(pltpu.VMEM)],
        out_specs=whole(pltpu.VMEM),
        scratch_shapes=[
            pltpu.VMEM(table.shape, f32),
            pltpu.VMEM((slots, width), f32),
        ],
        compiler_params=pltpu.CompilerParams(vmem_limit_bytes=VMEM_LIMIT),
        name="pool",
    )(rows, counts, ends, table)


def scatter_kernel(rows_ref, count_ref, ends_ref, fold_ref, table_ref, out_ref, spread, *sums):
    owners, slots = rows_ref.shape
    lanes_of = len(sums)
    for total in sums:
        total[...] = jnp.zeros_like(total)

    def owner(d, carry):
        members = members_of(ends_ref[pl.ds(d, 1), :], slots)
        spread[...] = jnp.dot(members, fold_ref[d], preferred_element_type=f32)

        def group(g, c):
            base = pl.multiple_of(g * 8, 8)
            block = spread[pl.ds(base, 8), :]
            for u in range(0, 8, lanes_of):
                spots = [rows_ref[d, base + u + v] for v in range(lanes_of)]
                news = [
                    sums[v][pl.ds(spots[v], 1), :] + block[u + v : u + v + 1]
                    for v in range(lanes_of)
                ]
                for v in range(lanes_of):
                    sums[v][pl.ds(spots[v], 1), :] = news[v]
            return c

        lax.fori_loop(0, (count_ref[d] + 7) // 8, group, 0)
        return carry

    lax.fori_loop(0, owners, owner, 0)
    step = 256

    def finish(g, c):
        at = pl.ds(pl.multiple_of(g * step, step), step)
        total = sums[0][at, :]
        for other in sums[1:]:
            total = total + other[at, :]
        out_ref[at, :] = (table_ref[at, :].astype(f32) - step_size * total).astype(bf16)
        return c

    lax.fori_loop(0, table_ref.shape[0] // step, finish, 0)


def scatter(rows, counts, ends, fold, table):
    slots = rows.shape[1]
    return pl.pallas_call(
        scatter_kernel,
        out_shape=jax.ShapeDtypeStruct(table.shape, bf16),
        in_specs=[whole(pltpu.SMEM), whole(pltpu.SMEM)] + [whole(pltpu.VMEM)] * 3,
        out_specs=whole(pltpu.VMEM),
        scratch_shapes=[pltpu.VMEM((slots, table.shape[1]), f32)]
        + [pltpu.VMEM(table.shape, f32)] * 4,
        compiler_params=pltpu.CompilerParams(vmem_limit_bytes=VMEM_LIMIT),
        name="scatter",
    )(rows, counts, ends, fold, table)


def small_kernel(part_rows, first_ref, ids_ref, grads_ref, table_ref, out_ref):
    senders, batch = ids_ref.shape
    rows = iota((part_rows, batch), 0) + first_ref[0]
    total = jnp.zeros(out_ref.shape, f32)

    def one(s, total):
        hot = (rows == ids_ref[pl.ds(s, 1), :]).astype(f32).astype(bf16)
        return total + jnp.dot(hot, grads_ref[s], preferred_element_type=f32)

    total = lax.fori_loop(0, senders, one, total)
    out_ref[...] = (table_ref[...].astype(f32) - step_size * total).astype(bf16)


def small_update(first, ids, grads, rows):
    return pl.pallas_call(
        functools.partial(small_kernel, rows.shape[0]),
        out_shape=jax.ShapeDtypeStruct(rows.shape, bf16),
        in_specs=[whole(pltpu.SMEM)] + [whole(pltpu.VMEM)] * 3,
        out_specs=whole(pltpu.VMEM),
        compiler_params=pltpu.CompilerParams(vmem_limit_bytes=VMEM_LIMIT),
        name="small_update",
    )(first, ids, grads, rows)


def spans_of(vec_count):
    return [(i, i * (i - 1) // 2) for i in range(1, vec_count)]


def top_kernel(
    vec_count, pad, sizes_ref, dense_ref, ids_ref, labels_ref, tables_ref, large_ref,
    w_ref, wd_ref, bias_ref, wout_ref, small_out, fold_out, vecs, gram, pairs, spread,
):
    batch, width = dense_ref.shape
    small_count, small_rows = tables_ref.shape[0], tables_ref.shape[1]
    feats, bag_span = large_ref.shape[0], large_ref.shape[1]
    pair_pad = pairs.shape[1]
    scale = width ** (-0.5)
    spans = spans_of(vec_count)

    def rows_of(i):
        return pl.ds(i, batch, stride=pad)

    vecs[rows_of(0), :] = dense_ref[...].astype(f32)
    rows = iota((batch, small_rows), 1)
    for t in range(small_count):
        hot = (ids_ref[:, t : t + 1] == rows).astype(f32).astype(bf16)
        vecs[rows_of(1 + t), :] = jnp.dot(hot, tables_ref[t], preferred_element_type=f32)
    sample = iota((batch, bag_span), 0)
    bag = iota((batch, bag_span), 1) * batch
    for f in range(feats):
        reach = sample * sizes_ref[f]
        hot = ((reach >= bag) & (reach < bag + batch)).astype(f32).astype(bf16)
        vecs[rows_of(1 + small_count + f), :] = jnp.dot(
            hot, large_ref[f], preferred_element_type=f32
        )
    for i in range(vec_count, pad):
        vecs[rows_of(i), :] = jnp.zeros((batch, width), f32)

    unroll = 8

    def gram_step(g, c):
        for u in range(unroll):
            at = pl.ds(pl.multiple_of((g * unroll + u) * pad, 8), pad)
            own = vecs[at, :].astype(bf16)
            gram[at, 0:pad] = lax.dot_general(
                own, own, (((1,), (1,)), ((), ())), preferred_element_type=f32
            )
        return c

    lax.fori_loop(0, batch // unroll, gram_step, 0)

    lane = iota((1, LANES), 1)
    chunk = 64
    for start in range(0, batch, chunk):
        tile = jnp.zeros((chunk, LANES), f32)
        at_tile = 0
        for i, off in spans:
            piece = gram[pl.ds(start * pad + i, chunk, stride=pad), :]
            turn = off % LANES
            if turn:
                piece = pltpu.roll(piece, turn, 1)
            low = off - at_tile * LANES
            tile = jnp.where((lane >= low) & (lane < low + i), piece, tile)
            if low + i >= LANES:
                pairs[start : start + chunk, at_tile * LANES : (at_tile + 1) * LANES] = (
                    tile * scale
                ).astype(bf16)
                at_tile += 1
                rest = low + i - LANES
                tile = jnp.where(lane < rest, piece, jnp.zeros_like(piece))
        if at_tile * LANES < pair_pad:
            pairs[start : start + chunk, at_tile * LANES : pair_pad] = (tile * scale).astype(bf16)

    block = 128
    for start in range(0, batch, block):
        at = slice(start, start + block)
        preact = (
            jnp.dot(pairs[at, :], w_ref[0:pair_pad, :], preferred_element_type=f32)
            + jnp.dot(dense_ref[at, :], wd_ref[...], preferred_element_type=f32)
            + bias_ref[...]
        )
        squash = jax.nn.sigmoid(preact)
        logits = jnp.sum(preact * squash * wout_ref[...], axis=1, keepdims=True)
        grad = jax.nn.sigmoid(logits) - labels_ref[at, :].astype(f32)
        pre_grad = (
            grad * wout_ref[...] * (squash * (1.0 + preact * (1.0 - squash)))
        ).astype(bf16)
        for q in range(0, pair_pad, LANES):
            spread[at, q : q + LANES] = lax.dot_general(
                pre_grad, w_ref[q : q + LANES, :], (((1,), (1,)), ((), ())),
                preferred_element_type=f32,
            ) * scale

    gram[rows_of(0), :] = jnp.zeros((batch, LANES), f32)
    for i in range(vec_count, pad):
        gram[rows_of(i), :] = jnp.zeros((batch, LANES), f32)
    for start in range(0, batch, chunk):
        for i, off in spans:
            first = off // LANES
            low = off - first * LANES
            here = spread[start : start + chunk, first * LANES : (first + 1) * LANES]
            if low + i > LANES:
                after = spread[start : start + chunk, (first + 1) * LANES : (first + 2) * LANES]
                here = jnp.where(lane >= low, here, after)
            if low:
                here = pltpu.roll(here, LANES - low, 1)
            gram[pl.ds(start * pad + i, chunk, stride=pad), :] = jnp.where(lane < i, here, 0.0)

    def back_step(g, c):
        for u in range(unroll):
            at = pl.ds(pl.multiple_of((g * unroll + u) * pad, 8), pad)
            lower = gram[at, :]
            both = lower[:, 0:pad] + jnp.transpose(lower)[0:pad, :]
            vecs[at, :] = jnp.dot(
                both.astype(bf16), vecs[at, :].astype(bf16), preferred_element_type=f32
            )
        return c

    lax.fori_loop(0, batch // unroll, back_step, 0)

    for t in range(small_count):
        small_out[t] = vecs[rows_of(1 + t), :].astype(bf16)
    sample_lane = iota((bag_span, batch), 1)
    bag_row = iota((bag_span, batch), 0) * batch
    for f in range(feats):
        reach = sample_lane * sizes_ref[f]
        hot = ((reach >= bag_row) & (reach < bag_row + batch)).astype(f32).astype(bf16)
        fold_out[f] = jnp.dot(
            hot, vecs[rows_of(1 + small_count + f), :].astype(bf16), preferred_element_type=f32
        ).astype(bf16)


def top(sizes, dense, ids, labels, tables, large, w_first, bias, wout):
    batch, width = dense.shape
    small_count, feats, bag_span = tables.shape[0], large.shape[0], large.shape[1]
    vec_count = 1 + small_count + feats
    pad = -(-vec_count // 8) * 8
    pair_count = vec_count * (vec_count - 1) // 2
    pair_pad = -(-pair_count // LANES) * LANES
    return pl.pallas_call(
        functools.partial(top_kernel, vec_count, pad),
        out_shape=(
            jax.ShapeDtypeStruct((small_count, batch, width), bf16),
            jax.ShapeDtypeStruct((feats, bag_span, width), bf16),
        ),
        in_specs=[whole(pltpu.SMEM)] + [whole(pltpu.VMEM)] * 9,
        out_specs=(whole(pltpu.VMEM), whole(pltpu.VMEM)),
        scratch_shapes=[
            pltpu.VMEM((batch * pad, width), f32),
            pltpu.VMEM((batch * pad, LANES), f32),
            pltpu.VMEM((batch, pair_pad), bf16),
            pltpu.VMEM((batch, pair_pad), f32),
        ],
        compiler_params=pltpu.CompilerParams(vmem_limit_bytes=VMEM_LIMIT),
        name="top",
    )(
        sizes, dense, ids, labels[:, None], tables, large, w_first, w_first[pair_count:],
        bias[None, :], wout[None, :],
    )


def shards(
    dense, small_ids, labels, small_tables, large_tables, batch_sizes, bag_ends,
    owner_row_index, w_first, b_first, w_out,
):
    groups = lax.axis_size("shard")
    copies = lax.axis_size("rep")
    replica = lax.axis_index("rep")
    member = lax.axis_index("shard")
    devices = groups * copies
    index = replica * groups + member
    small_count, small_rows, width = small_tables.shape
    batch = dense.shape[0]
    per_table = devices // small_count

    ids_by_table = jnp.transpose(small_ids)
    sent_ids = jnp.repeat(ids_by_table, per_table, axis=0)
    all_ids = lax.all_to_all(sent_ids, ("rep", "shard"), split_axis=0, concat_axis=0, tiled=True)

    ends, rows, table = bag_ends[0], owner_row_index[0], large_tables[0]
    counts = ends[:, -1]
    first = replica * groups

    def mine(x):
        return lax.dynamic_slice_in_dim(x, first, groups, 0)

    pooled = pool(mine(rows), mine(counts), mine(ends), table)
    large = lax.all_to_all(pooled, "shard", split_axis=0, concat_axis=0, tiled=True)
    sizes = lax.dynamic_slice_in_dim(batch_sizes, index, 1, 1)[:, 0]
    small_grads, fold = top(
        sizes, dense, small_ids, labels, small_tables, large, w_first, b_first, w_out
    )
    fold_back = lax.all_to_all(fold, "shard", split_axis=0, concat_axis=0, tiled=True)
    fold_all = lax.all_gather(fold_back, "rep", axis=0, tiled=True)
    sent = jnp.repeat(small_grads, per_table, axis=0)
    arrived = lax.all_to_all(sent, ("rep", "shard"), split_axis=0, concat_axis=0, tiled=True)
    part_rows = small_count * small_rows // devices
    flat = small_tables.reshape(small_count * small_rows, width)
    own = lax.dynamic_slice_in_dim(flat, index * part_rows, part_rows, 0)
    first_row = (lax.rem(index, per_table) * part_rows)[None].astype(jnp.int32)
    updated = small_update(first_row, all_ids, arrived, own)
    small_new = lax.all_gather(updated, ("rep", "shard"), axis=0, tiled=True).reshape(
        small_count, small_rows, width
    )
    large_new = scatter(rows, counts, ends, fold_all, table)
    return small_new, large_new[None]


def solution(mesh):
    both = ("rep", "shard")
    placed = (
        P(both, None), P(both, None), P(both), P(), P("shard", None, None), P(),
        P("shard", None, None), P("shard", None, None), P(), P(), P(),
    )
    return jax.shard_map(
        shards, mesh=mesh, in_specs=placed, out_specs=(P(), P("shard", None, None)), check_vma=False
    )
```

```python
import functools

import jax
import jax.numpy as jnp
from jax import lax
from jax.experimental import pallas as pl
from jax.experimental.pallas import tpu as pltpu
from jax.sharding import PartitionSpec as P

step_size = 32.0
LANES = 128
VMEM_LIMIT = 60 * 1024 * 1024
f32 = jnp.float32
bf16 = jnp.bfloat16


def whole(space):
    return pl.BlockSpec(memory_space=space)


def iota(shape, axis):
    return lax.broadcasted_iota(jnp.int32, shape, axis)


def members_of(ends, slots):
    span = ends.shape[-1]
    starts = jnp.where(iota((1, span), 1) == 0, 0, pltpu.roll(ends, 1, 1))
    places = iota((slots, span), 0)
    return ((places >= starts) & (places < ends)).astype(f32).astype(bf16)


def pool_kernel(first_ref, rows_ref, count_ref, ends_ref, table_ref, out_ref, wide, picked):
    slots = rows_ref.shape[1]
    owners = out_ref.shape[0]
    last = count_ref.shape[1] - 1
    first = first_ref[0]
    wide[...] = table_ref[...].astype(f32)
    picked[...] = jnp.zeros_like(picked)

    def owner(o, carry):
        d = o + first

        def group(g, c):
            base = pl.multiple_of(g * 8, 8)
            parts = [wide[pl.ds(rows_ref[d, base + u], 1), :] for u in range(8)]
            picked[pl.ds(base, 8), :] = jnp.concatenate(parts, axis=0)
            return c

        lax.fori_loop(0, (count_ref[d, last] + 7) // 8, group, 0)
        members = members_of(ends_ref[pl.ds(d, 1), :], slots)
        pooled = lax.dot_general(
            members, picked[...].astype(bf16), (((0,), (0,)), ((), ())),
            preferred_element_type=f32,
        )
        out_ref[o] = pooled.astype(bf16)
        return carry

    lax.fori_loop(0, owners, owner, 0)


def pool(first, owners, rows, ends, table):
    slots = rows.shape[1]
    width = table.shape[1]
    return pl.pallas_call(
        pool_kernel,
        out_shape=jax.ShapeDtypeStruct((owners, ends.shape[1], width), bf16),
        in_specs=[whole(pltpu.SMEM)] * 3 + [whole(pltpu.VMEM)] * 2,
        out_specs=whole(pltpu.VMEM),
        scratch_shapes=[
            pltpu.VMEM(table.shape, f32),
            pltpu.VMEM((slots, width), f32),
        ],
        compiler_params=pltpu.CompilerParams(vmem_limit_bytes=VMEM_LIMIT),
        name="pool",
    )(first, rows, ends, ends, table)


def scatter_kernel(rows_ref, count_ref, ends_ref, fold_ref, table_ref, out_ref, spread, *sums):
    owners, slots = rows_ref.shape
    last = count_ref.shape[1] - 1
    lanes_of = len(sums)
    for total in sums:
        total[...] = jnp.zeros_like(total)

    def owner(d, carry):
        members = members_of(ends_ref[pl.ds(d, 1), :], slots)
        spread[...] = jnp.dot(members, fold_ref[d], preferred_element_type=f32)

        def group(g, c):
            base = pl.multiple_of(g * 8, 8)
            block = spread[pl.ds(base, 8), :]
            for u in range(0, 8, lanes_of):
                spots = [rows_ref[d, base + u + v] for v in range(lanes_of)]
                news = [
                    sums[v][pl.ds(spots[v], 1), :] + block[u + v : u + v + 1]
                    for v in range(lanes_of)
                ]
                for v in range(lanes_of):
                    sums[v][pl.ds(spots[v], 1), :] = news[v]
            return c

        lax.fori_loop(0, (count_ref[d, last] + 7) // 8, group, 0)
        return carry

    lax.fori_loop(0, owners, owner, 0)
    step = 256

    def finish(g, c):
        at = pl.ds(pl.multiple_of(g * step, step), step)
        total = sums[0][at, :]
        for other in sums[1:]:
            total = total + other[at, :]
        out_ref[at, :] = (table_ref[at, :].astype(f32) - step_size * total).astype(bf16)
        return c

    lax.fori_loop(0, table_ref.shape[0] // step, finish, 0)


def scatter(rows, ends, fold, table):
    slots = rows.shape[1]
    return pl.pallas_call(
        scatter_kernel,
        out_shape=jax.ShapeDtypeStruct(table.shape, bf16),
        in_specs=[whole(pltpu.SMEM), whole(pltpu.SMEM)] + [whole(pltpu.VMEM)] * 3,
        out_specs=whole(pltpu.VMEM),
        scratch_shapes=[pltpu.VMEM((slots, table.shape[1]), f32)]
        + [pltpu.VMEM(table.shape, f32)] * 4,
        compiler_params=pltpu.CompilerParams(vmem_limit_bytes=VMEM_LIMIT),
        cost_estimate=pl.CostEstimate(
            flops=20 * table.size * LANES, bytes_accessed=4 * table.size, transcendentals=0
        ),
        name="scatter",
    )(rows, ends, ends, fold, table)


def small_kernel(part_rows, first_ref, ids_ref, grads_ref, table_ref, out_ref):
    senders, batch = ids_ref.shape
    rows = iota((part_rows, batch), 0) + first_ref[0]
    total = jnp.zeros(out_ref.shape, f32)

    def one(s, total):
        hot = (rows == ids_ref[pl.ds(s, 1), :]).astype(f32).astype(bf16)
        return total + jnp.dot(hot, grads_ref[s], preferred_element_type=f32)

    total = lax.fori_loop(0, senders, one, total)
    out_ref[...] = (table_ref[...].astype(f32) - step_size * total).astype(bf16)


def small_update(first, ids, grads, rows):
    return pl.pallas_call(
        functools.partial(small_kernel, rows.shape[0]),
        out_shape=jax.ShapeDtypeStruct(rows.shape, bf16),
        in_specs=[whole(pltpu.SMEM)] + [whole(pltpu.VMEM)] * 3,
        out_specs=whole(pltpu.VMEM),
        compiler_params=pltpu.CompilerParams(vmem_limit_bytes=VMEM_LIMIT),
        name="small_update",
    )(first, ids, grads, rows)


def spans_of(vec_count):
    return [(i, i * (i - 1) // 2) for i in range(1, vec_count)]


def top_kernel(
    vec_count, pad, index_ref, sizes_ref, dense_ref, ids_ref, labels_ref, tables_ref, large_ref,
    w_ref, bias_ref, wout_ref, small_out, fold_out, vecs, gram, pairs, spread,
):
    batch, width = dense_ref.shape
    small_count, small_rows = tables_ref.shape[0], tables_ref.shape[1]
    feats, bag_span = large_ref.shape[0], large_ref.shape[1]
    pair_pad = pairs.shape[1]
    pair_count = vec_count * (vec_count - 1) // 2
    scale = width ** (-0.5)
    spans = spans_of(vec_count)

    def rows_of(i):
        return pl.ds(i, batch, stride=pad)

    vecs[rows_of(0), :] = dense_ref[...].astype(f32)
    rows = iota((batch, small_rows), 1)
    for t in range(small_count):
        hot = (ids_ref[:, t : t + 1] == rows).astype(f32).astype(bf16)
        vecs[rows_of(1 + t), :] = jnp.dot(hot, tables_ref[t], preferred_element_type=f32)
    sample = iota((batch, bag_span), 0)
    bag = iota((batch, bag_span), 1) * batch
    for f in range(feats):
        reach = sample * sizes_ref[f, index_ref[0]]
        hot = ((reach >= bag) & (reach < bag + batch)).astype(f32).astype(bf16)
        vecs[rows_of(1 + small_count + f), :] = jnp.dot(
            hot, large_ref[f], preferred_element_type=f32
        )
    for i in range(vec_count, pad):
        vecs[rows_of(i), :] = jnp.zeros((batch, width), f32)

    unroll = 8

    def gram_step(g, c):
        for u in range(unroll):
            at = pl.ds(pl.multiple_of((g * unroll + u) * pad, 8), pad)
            own = vecs[at, :].astype(bf16)
            gram[at, 0:pad] = lax.dot_general(
                own, own, (((1,), (1,)), ((), ())), preferred_element_type=f32
            )
        return c

    lax.fori_loop(0, batch // unroll, gram_step, 0)

    lane = iota((1, LANES), 1)
    chunk = 64
    for start in range(0, batch, chunk):
        tile = jnp.zeros((chunk, LANES), f32)
        at_tile = 0
        for i, off in spans:
            piece = gram[pl.ds(start * pad + i, chunk, stride=pad), :]
            turn = off % LANES
            if turn:
                piece = pltpu.roll(piece, turn, 1)
            low = off - at_tile * LANES
            tile = jnp.where((lane >= low) & (lane < low + i), piece, tile)
            if low + i >= LANES:
                pairs[start : start + chunk, at_tile * LANES : (at_tile + 1) * LANES] = (
                    tile * scale
                ).astype(bf16)
                at_tile += 1
                rest = low + i - LANES
                tile = jnp.where(lane < rest, piece, jnp.zeros_like(piece))
        if at_tile * LANES < pair_pad:
            pairs[start : start + chunk, at_tile * LANES : pair_pad] = (tile * scale).astype(bf16)

    block = 128
    for start in range(0, batch, block):
        at = slice(start, start + block)
        preact = (
            jnp.dot(pairs[at, :], w_ref[0:pair_pad, :], preferred_element_type=f32)
            + jnp.dot(dense_ref[at, :], w_ref[pair_count : pair_count + width, :], preferred_element_type=f32)
            + bias_ref[...]
        )
        squash = jax.nn.sigmoid(preact)
        logits = jnp.sum(preact * squash * wout_ref[...], axis=1, keepdims=True)
        grad = jax.nn.sigmoid(logits) - labels_ref[at, :].astype(f32)
        pre_grad = (
            grad * wout_ref[...] * (squash * (1.0 + preact * (1.0 - squash)))
        ).astype(bf16)
        for q in range(0, pair_pad, LANES):
            spread[at, q : q + LANES] = lax.dot_general(
                pre_grad, w_ref[q : q + LANES, :], (((1,), (1,)), ((), ())),
                preferred_element_type=f32,
            ) * scale

    gram[rows_of(0), :] = jnp.zeros((batch, LANES), f32)
    for i in range(vec_count, pad):
        gram[rows_of(i), :] = jnp.zeros((batch, LANES), f32)
    for start in range(0, batch, chunk):
        for i, off in spans:
            first = off // LANES
            low = off - first * LANES
            here = spread[start : start + chunk, first * LANES : (first + 1) * LANES]
            if low + i > LANES:
                after = spread[start : start + chunk, (first + 1) * LANES : (first + 2) * LANES]
                here = jnp.where(lane >= low, here, after)
            if low:
                here = pltpu.roll(here, LANES - low, 1)
            gram[pl.ds(start * pad + i, chunk, stride=pad), :] = jnp.where(lane < i, here, 0.0)

    def back_step(g, c):
        for u in range(unroll):
            at = pl.ds(pl.multiple_of((g * unroll + u) * pad, 8), pad)
            lower = gram[at, :]
            both = lower[:, 0:pad] + jnp.transpose(lower)[0:pad, :]
            vecs[at, :] = jnp.dot(
                both.astype(bf16), vecs[at, :].astype(bf16), preferred_element_type=f32
            )
        return c

    lax.fori_loop(0, batch // unroll, back_step, 0)

    for t in range(small_count):
        small_out[t] = vecs[rows_of(1 + t), :].astype(bf16)
    sample_lane = iota((bag_span, batch), 1)
    bag_row = iota((bag_span, batch), 0) * batch
    for f in range(feats):
        reach = sample_lane * sizes_ref[f, index_ref[0]]
        hot = ((reach >= bag_row) & (reach < bag_row + batch)).astype(f32).astype(bf16)
        fold_out[f] = jnp.dot(
            hot, vecs[rows_of(1 + small_count + f), :].astype(bf16), preferred_element_type=f32
        ).astype(bf16)


def top(index, sizes, dense, ids, labels, tables, large, w_first, bias, wout):
    batch, width = dense.shape
    small_count, feats, bag_span = tables.shape[0], large.shape[0], large.shape[1]
    vec_count = 1 + small_count + feats
    pad = -(-vec_count // 8) * 8
    pair_count = vec_count * (vec_count - 1) // 2
    pair_pad = -(-pair_count // LANES) * LANES
    return pl.pallas_call(
        functools.partial(top_kernel, vec_count, pad),
        out_shape=(
            jax.ShapeDtypeStruct((small_count, batch, width), bf16),
            jax.ShapeDtypeStruct((feats, bag_span, width), bf16),
        ),
        in_specs=[whole(pltpu.SMEM)] * 2 + [whole(pltpu.VMEM)] * 8,
        out_specs=(whole(pltpu.VMEM), whole(pltpu.VMEM)),
        scratch_shapes=[
            pltpu.VMEM((batch * pad, width), f32),
            pltpu.VMEM((batch * pad, LANES), f32),
            pltpu.VMEM((batch, pair_pad), bf16),
            pltpu.VMEM((batch, pair_pad), f32),
        ],
        compiler_params=pltpu.CompilerParams(vmem_limit_bytes=VMEM_LIMIT),
        name="top",
    )(
        index, sizes, dense, ids, labels[:, None], tables, large, w_first,
        bias[None, :], wout[None, :],
    )


def greet_all():
    copies, groups = lax.axis_size("rep"), lax.axis_size("shard")
    devices = copies * groups
    index = lax.axis_index("rep") * groups + lax.axis_index("shard")
    barrier = pltpu.get_barrier_semaphore()

    def greet(k, c):
        other = lax.rem(index + k, devices)
        pl.semaphore_signal(
            barrier, inc=1, device_id={"rep": other // groups, "shard": lax.rem(other, groups)},
            device_id_type=pl.DeviceIdType.MESH,
        )
        return c

    lax.fori_loop(1, devices, greet, 0)
    pl.semaphore_wait(barrier, devices - 1)


def remote(src, dst, send, recv, rep, shard):
    return pltpu.make_async_remote_copy(
        src_ref=src, dst_ref=dst, send_sem=send, recv_sem=recv,
        device_id={"rep": rep, "shard": shard}, device_id_type=pl.DeviceIdType.MESH,
    )


def forward_kernel(
    pooled_ref, ids_ref, large_out, ids_out, send, recv, id_send, id_recv, own
):
    copies, groups = lax.axis_size("rep"), lax.axis_size("shard")
    devices = copies * groups
    rep, me = lax.axis_index("rep"), lax.axis_index("shard")
    index = rep * groups + me

    def block(k):
        to = lax.rem(me + k, groups)
        return remote(pooled_ref.at[to], large_out.at[me], send.at[k], recv.at[k], rep, to)

    def ids(k):
        to = lax.rem(index + k, devices)
        return remote(
            ids_ref.at[to], ids_out.at[index], id_send.at[k], id_recv.at[k],
            to // groups, lax.rem(to, groups),
        )

    def block_in(k):
        at = lax.rem(me + groups - k, groups)
        return remote(pooled_ref.at[at], large_out.at[at], send.at[k], recv.at[k], rep, at)

    def ids_in(k):
        at = lax.rem(index + devices - k, devices)
        return remote(
            ids_ref.at[at], ids_out.at[at], id_send.at[k], id_recv.at[k],
            at // groups, lax.rem(at, groups),
        )

    def run(low, high, act):
        def body(k, c):
            act(k)
            return c

        lax.fori_loop(low, high, body, 0)

    greet_all()
    run(1, groups, lambda k: block(k).start())
    run(1, devices, lambda k: ids(k).start())
    mine = pltpu.make_async_copy(pooled_ref.at[me], large_out.at[me], own.at[0])
    mine_ids = pltpu.make_async_copy(ids_ref.at[index], ids_out.at[index], own.at[1])
    mine.start()
    mine_ids.start()
    mine.wait()
    mine_ids.wait()
    run(1, groups, lambda k: block_in(k).wait_recv())
    run(1, devices, lambda k: ids_in(k).wait_recv())
    run(1, groups, lambda k: block(k).wait_send())
    run(1, devices, lambda k: ids(k).wait_send())


def forward(pooled, ids):
    groups, devices = pooled.shape[0], ids.shape[0]
    return pl.pallas_call(
        forward_kernel,
        out_shape=(
            jax.ShapeDtypeStruct(pooled.shape, pooled.dtype),
            jax.ShapeDtypeStruct(ids.shape, ids.dtype),
        ),
        in_specs=[whole(pltpu.VMEM)] * 2,
        out_specs=(whole(pltpu.VMEM), whole(pltpu.VMEM)),
        scratch_shapes=[pltpu.SemaphoreType.DMA((groups,))] * 2
        + [pltpu.SemaphoreType.DMA((devices,))] * 2
        + [pltpu.SemaphoreType.DMA((2,))],
        compiler_params=pltpu.CompilerParams(
            collective_id=0, has_side_effects=True, vmem_limit_bytes=VMEM_LIMIT
        ),
        name="forward",
    )(pooled, ids)


def fold_kernel(fold_ref, out_ref, send, recv, far_send, far_recv, own):
    copies, groups = lax.axis_size("rep"), lax.axis_size("shard")
    rep, me = lax.axis_index("rep"), lax.axis_index("shard")
    other = 1 - rep

    def out_block(k):
        to = lax.rem(me + k, groups)
        return remote(
            fold_ref.at[to], out_ref.at[rep * groups + me], send.at[k], recv.at[k], rep, to
        )

    def in_block(k):
        at = lax.rem(me + groups - k, groups)
        return remote(
            fold_ref.at[at], out_ref.at[rep * groups + at], send.at[k], recv.at[k], rep, at
        )

    def far_out(k):
        slot = out_ref.at[rep * groups + lax.rem(me + groups - k, groups)]
        return remote(slot, slot, far_send.at[k], far_recv.at[k], other, me)

    def far_in(k):
        slot = out_ref.at[other * groups + lax.rem(me + groups - k, groups)]
        return remote(slot, slot, far_send.at[k], far_recv.at[k], other, me)

    own_far = remote(
        fold_ref.at[me], out_ref.at[rep * groups + me], far_send.at[0], far_recv.at[0], other, me
    )

    def run(act):
        def body(k, c):
            act(k)
            return c

        lax.fori_loop(1, groups, body, 0)

    greet_all()
    run(lambda k: out_block(k).start())
    own_far.start()
    mine = pltpu.make_async_copy(fold_ref.at[me], out_ref.at[rep * groups + me], own.at[0])
    mine.start()

    def pass_on(k):
        in_block(k).wait_recv()
        far_out(k).start()

    run(pass_on)
    mine.wait()
    far_in(0).wait_recv()
    run(lambda k: far_in(k).wait_recv())
    own_far.wait_send()
    run(lambda k: far_out(k).wait_send())
    run(lambda k: out_block(k).wait_send())


def fold_exchange(fold, copies):
    groups = fold.shape[0]
    return pl.pallas_call(
        fold_kernel,
        out_shape=jax.ShapeDtypeStruct((copies * groups,) + fold.shape[1:], fold.dtype),
        in_specs=[whole(pltpu.VMEM)],
        out_specs=whole(pltpu.VMEM),
        scratch_shapes=[pltpu.SemaphoreType.DMA((groups,))] * 4 + [pltpu.SemaphoreType.DMA((1,))],
        compiler_params=pltpu.CompilerParams(
            collective_id=1, has_side_effects=True, vmem_limit_bytes=VMEM_LIMIT
        ),
        name="fold_exchange",
    )(fold)


def spread_kernel(own_ref, out_ref, send_z, send_1, send_2, send_core, recv, local):
    groups = lax.axis_size("shard")
    ring = groups // 4
    rep, member = lax.axis_index("rep"), lax.axis_index("shard")
    z, y, core = member // 4, lax.rem(member, 4) // 2, lax.rem(member, 2)

    def shard_of(z_at, y_at, core_at):
        return z_at * 4 + y_at * 2 + core_at

    def send(h, src, rep_at, z_at, y_at, sem, to_rep, to_z, to_y, to_core):
        slot = rep_at * groups + shard_of(z_at, y_at, core)
        source = out_ref.at[slot, h] if src is None else src
        return remote(
            source, out_ref.at[slot, h], sem, recv.at[h, slot],
            to_rep, shard_of(to_z, to_y, to_core),
        )

    def arrived(h, rep_at, z_at, y_at, core_at):
        slot = rep_at * groups + shard_of(z_at, y_at, core_at)
        place = out_ref.at[slot, h]
        remote(place, place, local.at[1], recv.at[h, slot], rep, member).wait_recv()

    greet_all()
    pending = []

    def go(copy):
        copy.start()
        pending.append(copy)

    def second(h, k, src, rep_at, z_at, y_at):
        hop = (rep, z, 1 - y, core) if h == 0 else (1 - rep, z, y, core)
        go(send(h, src, rep_at, z_at, y_at, send_1.at[h, k], *hop))

    def third(h, k, src, rep_at, z_at, y_at):
        hop = (1 - rep, z, y, core) if h == 0 else (rep, z, 1 - y, core)
        go(send(h, src, rep_at, z_at, y_at, send_2.at[h, k], *hop))

    def last(h, k, src, rep_at, z_at, y_at):
        go(send(h, src, rep_at, z_at, y_at, send_core.at[h, k], rep, z, y, 1 - core))

    for k in range(1, ring):
        for h in range(2):
            go(send(h, own_ref.at[h], rep, z, y, send_z.at[h, k], rep, lax.rem(z + k, ring), y, core))
    for h in range(2):
        src = own_ref.at[h]
        second(h, 0, src, rep, z, y)
        third(h, 0, src, rep, z, y)
        last(h, 0, src, rep, z, y)
    mine = pltpu.make_async_copy(
        own_ref, out_ref.at[rep * groups + member], local.at[0]
    )
    mine.start()
    for k in range(1, ring):
        z_at = lax.rem(z + ring - k, ring)
        for h in range(2):
            arrived(h, rep, z_at, y, core)
            second(h, k, None, rep, z_at, y)
            third(h, k, None, rep, z_at, y)
            last(h, k, None, rep, z_at, y)
    for k in range(ring):
        z_at = lax.rem(z + ring - k, ring)
        for h in range(2):
            where = (rep, z_at, 1 - y) if h == 0 else (1 - rep, z_at, y)
            arrived(h, *where, core)
            third(h, ring + k, None, *where)
            last(h, ring + k, None, *where)
    for k in range(2 * ring):
        z_at = lax.rem(z + ring - k % ring, ring)
        for h in range(2):
            if h == 0:
                where = (1 - rep, z_at, y if k < ring else 1 - y)
            else:
                where = (rep if k < ring else 1 - rep, z_at, 1 - y)
            arrived(h, *where, core)
            last(h, 2 * ring + k, None, *where)
    for r in range(2):
        for k in range(ring):
            for y_at in range(2):
                for h in range(2):
                    arrived(h, r, k, y_at, 1 - core)
    mine.wait()
    for copy in pending:
        copy.wait_send()


def spread_all(own, copies, groups):
    rows, width = own.shape
    ring = groups // 4
    devices = copies * groups
    out = pl.pallas_call(
        spread_kernel,
        out_shape=jax.ShapeDtypeStruct((devices, 2, rows // 2, width), own.dtype),
        in_specs=[whole(pltpu.VMEM)],
        out_specs=whole(pltpu.VMEM),
        scratch_shapes=[
            pltpu.SemaphoreType.DMA((2, ring)),
            pltpu.SemaphoreType.DMA((2, ring)),
            pltpu.SemaphoreType.DMA((2, 2 * ring)),
            pltpu.SemaphoreType.DMA((2, 4 * ring)),
            pltpu.SemaphoreType.DMA((2, devices)),
            pltpu.SemaphoreType.DMA((2,)),
        ],
        compiler_params=pltpu.CompilerParams(
            collective_id=2, has_side_effects=True, vmem_limit_bytes=VMEM_LIMIT
        ),
        name="spread_all",
    )(own.reshape(2, rows // 2, width))
    return out.reshape(devices * rows, width)


def shards(
    dense, small_ids, labels, small_tables, large_tables, batch_sizes, bag_ends,
    owner_row_index, w_first, b_first, w_out,
):
    groups = lax.axis_size("shard")
    copies = lax.axis_size("rep")
    devices = groups * copies
    first = lax.axis_index("rep") * groups
    index = first + lax.axis_index("shard")
    small_count, small_rows, width = small_tables.shape
    per_table = devices // small_count
    ends, rows, table = bag_ends[0], owner_row_index[0], large_tables[0]

    sent_ids = jnp.repeat(jnp.transpose(small_ids), per_table, axis=0)[:, None]
    pooled = pool(first[None], groups, rows, ends, table)
    large, all_ids = forward(pooled, sent_ids)
    small_grads, fold = top(
        index[None], batch_sizes, dense, small_ids, labels, small_tables, large, w_first,
        b_first, w_out,
    )
    fold_all = fold_exchange(fold, copies)
    sent = jnp.repeat(small_grads, per_table, axis=0)
    sent, fold_all = lax.optimization_barrier((sent, fold_all))
    arrived = lax.all_to_all(sent, ("rep", "shard"), split_axis=0, concat_axis=0, tiled=True)
    large_new = scatter(rows, ends, fold_all, table)
    part_rows = small_count * small_rows // devices
    flat = small_tables.reshape(small_count * small_rows, width)
    own = lax.dynamic_slice_in_dim(flat, index * part_rows, part_rows, 0)
    first_row = (lax.rem(index, per_table) * part_rows)[None].astype(jnp.int32)
    updated = small_update(first_row, all_ids[:, 0], arrived, own)
    small_new = spread_all(updated, copies, groups).reshape(small_count, small_rows, width)
    return small_new, large_new[None]


def solution(mesh):
    both = ("rep", "shard")
    placed = (
        P(both, None), P(both, None), P(both), P(), P("shard", None, None), P(),
        P("shard", None, None), P("shard", None, None), P(), P(), P(),
    )
    return jax.shard_map(
        shards, mesh=mesh, in_specs=placed, out_specs=(P(), P("shard", None, None)), check_vma=False
    )
```

```python
import functools

import jax
import jax.numpy as jnp
from jax import lax
from jax.experimental import pallas as pl
from jax.experimental.pallas import tpu as pltpu
from jax.sharding import PartitionSpec as P

step_size = 32.0
LANES = 128
VMEM_LIMIT = 60 * 1024 * 1024
f32 = jnp.float32
bf16 = jnp.bfloat16


def whole(space):
    return pl.BlockSpec(memory_space=space)


def iota(shape, axis):
    return lax.broadcasted_iota(jnp.int32, shape, axis)


def members_of(ends, slots):
    span = ends.shape[-1]
    starts = jnp.where(iota((1, span), 1) == 0, 0, pltpu.roll(ends, 1, 1))
    places = iota((slots, span), 0)
    return ((places >= starts) & (places < ends)).astype(f32).astype(bf16)


def pool_kernel(first_ref, rows_ref, count_ref, ends_ref, table_ref, out_ref, wide, picked):
    slots = rows_ref.shape[1]
    owners = out_ref.shape[0]
    last = count_ref.shape[1] - 1
    first = first_ref[0]
    wide[...] = table_ref[...].astype(f32)
    picked[...] = jnp.zeros_like(picked)

    def owner(o, carry):
        d = o + first

        def group(g, c):
            base = pl.multiple_of(g * 8, 8)
            parts = [wide[pl.ds(rows_ref[d, base + u], 1), :] for u in range(8)]
            picked[pl.ds(pl.multiple_of(o * slots + base, 8), 8), :] = jnp.concatenate(parts, axis=0)
            return c

        return lax.fori_loop(0, (count_ref[d, last] + 7) // 8, group, carry)

    lax.fori_loop(0, owners, owner, 0)

    def sums(o, carry):
        members = members_of(ends_ref[pl.ds(o + first, 1), :], slots)
        block = picked[pl.ds(pl.multiple_of(o * slots, 8), slots), :].astype(bf16)
        pooled = lax.dot_general(
            members, block, (((0,), (0,)), ((), ())), preferred_element_type=f32
        )
        out_ref[o] = pooled.astype(bf16)
        return carry

    lax.fori_loop(0, owners, sums, 0, unroll=4)


def pool(first, owners, rows, ends, table):
    slots = rows.shape[1]
    width = table.shape[1]
    return pl.pallas_call(
        pool_kernel,
        out_shape=jax.ShapeDtypeStruct((owners, ends.shape[1], width), bf16),
        in_specs=[whole(pltpu.SMEM)] * 3 + [whole(pltpu.VMEM)] * 2,
        out_specs=whole(pltpu.VMEM),
        scratch_shapes=[
            pltpu.VMEM(table.shape, f32),
            pltpu.VMEM((owners * slots, width), f32),
        ],
        compiler_params=pltpu.CompilerParams(vmem_limit_bytes=VMEM_LIMIT),
        name="pool",
    )(first, rows, ends, ends, table)


def scatter_kernel(rows_ref, count_ref, ends_ref, fold_ref, table_ref, out_ref, spread, *sums):
    owners, slots = rows_ref.shape
    last = count_ref.shape[1] - 1
    lanes_of = len(sums)
    for total in sums:
        total[...] = jnp.zeros_like(total)

    def expand(d, carry):
        members = members_of(ends_ref[pl.ds(d, 1), :], slots)
        spread[pl.ds(pl.multiple_of(d * slots, 8), slots), :] = jnp.dot(
            members, fold_ref[d], preferred_element_type=f32
        )
        return carry

    lax.fori_loop(0, owners, expand, 0, unroll=4)

    def owner(d, carry):
        def group(g, c):
            base = pl.multiple_of(g * 8, 8)
            block = spread[pl.ds(pl.multiple_of(d * slots + base, 8), 8), :]
            for u in range(0, 8, lanes_of):
                spots = [rows_ref[d, base + u + v] for v in range(lanes_of)]
                news = [
                    sums[v][pl.ds(spots[v], 1), :] + block[u + v : u + v + 1]
                    for v in range(lanes_of)
                ]
                for v in range(lanes_of):
                    sums[v][pl.ds(spots[v], 1), :] = news[v]
            return c

        return lax.fori_loop(0, (count_ref[d, last] + 7) // 8, group, carry)

    lax.fori_loop(0, owners, owner, 0)
    step = 256

    def finish(g, c):
        at = pl.ds(pl.multiple_of(g * step, step), step)
        total = sums[0][at, :]
        for other in sums[1:]:
            total = total + other[at, :]
        out_ref[at, :] = (table_ref[at, :].astype(f32) - step_size * total).astype(bf16)
        return c

    lax.fori_loop(0, table_ref.shape[0] // step, finish, 0)


def scatter(rows, ends, fold, table):
    slots = rows.shape[1]
    return pl.pallas_call(
        scatter_kernel,
        out_shape=jax.ShapeDtypeStruct(table.shape, bf16),
        in_specs=[whole(pltpu.SMEM), whole(pltpu.SMEM)] + [whole(pltpu.VMEM)] * 3,
        out_specs=whole(pltpu.VMEM),
        scratch_shapes=[pltpu.VMEM((rows.size, table.shape[1]), f32)]
        + [pltpu.VMEM(table.shape, f32)] * 4,
        compiler_params=pltpu.CompilerParams(vmem_limit_bytes=VMEM_LIMIT),
        cost_estimate=pl.CostEstimate(
            flops=20 * table.size * LANES, bytes_accessed=4 * table.size, transcendentals=0
        ),
        name="scatter",
    )(rows, ends, ends, fold, table)


def small_kernel(part_rows, first_ref, ids_ref, grads_ref, table_ref, out_ref):
    senders, batch = ids_ref.shape
    rows = iota((part_rows, batch), 0) + first_ref[0]
    total = jnp.zeros(out_ref.shape, f32)

    def one(s, total):
        hot = (rows == ids_ref[pl.ds(s, 1), :]).astype(f32).astype(bf16)
        return total + jnp.dot(hot, grads_ref[s], preferred_element_type=f32)

    total = lax.fori_loop(0, senders, one, total, unroll=8)
    out_ref[...] = (table_ref[...].astype(f32) - step_size * total).astype(bf16)


def small_update(first, ids, grads, rows):
    return pl.pallas_call(
        functools.partial(small_kernel, rows.shape[0]),
        out_shape=jax.ShapeDtypeStruct(rows.shape, bf16),
        in_specs=[whole(pltpu.SMEM)] + [whole(pltpu.VMEM)] * 3,
        out_specs=whole(pltpu.VMEM),
        compiler_params=pltpu.CompilerParams(vmem_limit_bytes=VMEM_LIMIT),
        name="small_update",
    )(first, ids, grads, rows)


def spans_of(vec_count):
    return [(i, i * (i - 1) // 2) for i in range(1, vec_count)]


def top_kernel(
    vec_count, pad, index_ref, sizes_ref, dense_ref, labels_ref, small_ref, large_ref,
    w_ref, bias_ref, wout_ref, small_out, fold_out, vecs, gram, pairs, spread,
):
    batch, width = dense_ref.shape
    small_count = small_ref.shape[0]
    feats, bag_span = large_ref.shape[0], large_ref.shape[1]
    pair_pad = pairs.shape[1]
    pair_count = vec_count * (vec_count - 1) // 2
    scale = width ** (-0.5)
    spans = spans_of(vec_count)

    def rows_of(i):
        return pl.ds(i, batch, stride=pad)

    vecs[rows_of(0), :] = dense_ref[...].astype(f32)
    for t in range(small_count):
        vecs[rows_of(1 + t), :] = small_ref[t].astype(f32)
    sample = iota((batch, bag_span), 0)
    bag = iota((batch, bag_span), 1) * batch
    for f in range(feats):
        reach = sample * sizes_ref[f, index_ref[0]]
        hot = ((reach >= bag) & (reach < bag + batch)).astype(f32).astype(bf16)
        vecs[rows_of(1 + small_count + f), :] = jnp.dot(
            hot, large_ref[f], preferred_element_type=f32
        )
    for i in range(vec_count, pad):
        vecs[rows_of(i), :] = jnp.zeros((batch, width), f32)

    unroll = 8

    def gram_step(g, c):
        for u in range(unroll):
            at = pl.ds(pl.multiple_of((g * unroll + u) * pad, 8), pad)
            own = vecs[at, :].astype(bf16)
            gram[at, 0:pad] = lax.dot_general(
                own, own, (((1,), (1,)), ((), ())), preferred_element_type=f32
            )
        return c

    lax.fori_loop(0, batch // unroll, gram_step, 0)

    lane = iota((1, LANES), 1)
    chunk = 64
    for start in range(0, batch, chunk):
        tile = jnp.zeros((chunk, LANES), f32)
        at_tile = 0
        for i, off in spans:
            piece = gram[pl.ds(start * pad + i, chunk, stride=pad), :]
            turn = off % LANES
            if turn:
                piece = pltpu.roll(piece, turn, 1)
            low = off - at_tile * LANES
            tile = jnp.where((lane >= low) & (lane < low + i), piece, tile)
            if low + i >= LANES:
                pairs[start : start + chunk, at_tile * LANES : (at_tile + 1) * LANES] = (
                    tile * scale
                ).astype(bf16)
                at_tile += 1
                rest = low + i - LANES
                tile = jnp.where(lane < rest, piece, jnp.zeros_like(piece))
        if at_tile * LANES < pair_pad:
            pairs[start : start + chunk, at_tile * LANES : pair_pad] = (tile * scale).astype(bf16)

    block = 128
    for start in range(0, batch, block):
        at = slice(start, start + block)
        preact = (
            jnp.dot(pairs[at, :], w_ref[0:pair_pad, :], preferred_element_type=f32)
            + jnp.dot(dense_ref[at, :], w_ref[pair_count : pair_count + width, :], preferred_element_type=f32)
            + bias_ref[...]
        )
        squash = jax.nn.sigmoid(preact)
        logits = jnp.sum(preact * squash * wout_ref[...], axis=1, keepdims=True)
        grad = jax.nn.sigmoid(logits) - labels_ref[at, :].astype(f32)
        pre_grad = (
            grad * wout_ref[...] * (squash * (1.0 + preact * (1.0 - squash)))
        ).astype(bf16)
        for q in range(0, pair_pad, LANES):
            spread[at, q : q + LANES] = lax.dot_general(
                pre_grad, w_ref[q : q + LANES, :], (((1,), (1,)), ((), ())),
                preferred_element_type=f32,
            ) * scale

    gram[rows_of(0), :] = jnp.zeros((batch, LANES), f32)
    for i in range(vec_count, pad):
        gram[rows_of(i), :] = jnp.zeros((batch, LANES), f32)
    for start in range(0, batch, chunk):
        for i, off in spans:
            first = off // LANES
            low = off - first * LANES
            here = spread[start : start + chunk, first * LANES : (first + 1) * LANES]
            if low + i > LANES:
                after = spread[start : start + chunk, (first + 1) * LANES : (first + 2) * LANES]
                here = jnp.where(lane >= low, here, after)
            if low:
                here = pltpu.roll(here, LANES - low, 1)
            gram[pl.ds(start * pad + i, chunk, stride=pad), :] = jnp.where(lane < i, here, 0.0)

    def back_step(g, c):
        for u in range(unroll):
            at = pl.ds(pl.multiple_of((g * unroll + u) * pad, 8), pad)
            lower = gram[at, :]
            both = lower[:, 0:pad] + jnp.transpose(lower)[0:pad, :]
            vecs[at, :] = jnp.dot(
                both.astype(bf16), vecs[at, :].astype(bf16), preferred_element_type=f32
            )
        return c

    lax.fori_loop(0, batch // unroll, back_step, 0)

    for t in range(small_count):
        small_out[t] = vecs[rows_of(1 + t), :].astype(bf16)
    sample_lane = iota((bag_span, batch), 1)
    bag_row = iota((bag_span, batch), 0) * batch
    for f in range(feats):
        reach = sample_lane * sizes_ref[f, index_ref[0]]
        hot = ((reach >= bag_row) & (reach < bag_row + batch)).astype(f32).astype(bf16)
        fold_out[f] = jnp.dot(
            hot, vecs[rows_of(1 + small_count + f), :].astype(bf16), preferred_element_type=f32
        ).astype(bf16)


def top(index, sizes, dense, labels, small, large, w_first, bias, wout):
    batch, width = dense.shape
    small_count, feats, bag_span = small.shape[0], large.shape[0], large.shape[1]
    vec_count = 1 + small_count + feats
    pad = -(-vec_count // 8) * 8
    pair_count = vec_count * (vec_count - 1) // 2
    pair_pad = -(-pair_count // LANES) * LANES
    return pl.pallas_call(
        functools.partial(top_kernel, vec_count, pad),
        out_shape=(
            jax.ShapeDtypeStruct((small_count, batch, width), bf16),
            jax.ShapeDtypeStruct((feats, bag_span, width), bf16),
        ),
        in_specs=[whole(pltpu.SMEM)] * 2 + [whole(pltpu.VMEM)] * 7,
        out_specs=(whole(pltpu.VMEM), whole(pltpu.VMEM)),
        scratch_shapes=[
            pltpu.VMEM((batch * pad, width), f32),
            pltpu.VMEM((batch * pad, LANES), f32),
            pltpu.VMEM((batch, pair_pad), bf16),
            pltpu.VMEM((batch, pair_pad), f32),
        ],
        compiler_params=pltpu.CompilerParams(vmem_limit_bytes=VMEM_LIMIT),
        name="top",
    )(
        index, sizes, dense, labels[:, None], small, large, w_first,
        bias[None, :], wout[None, :],
    )


def greet_all():
    copies, groups = lax.axis_size("rep"), lax.axis_size("shard")
    devices = copies * groups
    index = lax.axis_index("rep") * groups + lax.axis_index("shard")
    barrier = pltpu.get_barrier_semaphore()

    def greet(k, c):
        other = lax.rem(index + k, devices)
        pl.semaphore_signal(
            barrier, inc=1, device_id={"rep": other // groups, "shard": lax.rem(other, groups)},
            device_id_type=pl.DeviceIdType.MESH,
        )
        return c

    lax.fori_loop(1, devices, greet, 0)
    pl.semaphore_wait(barrier, devices - 1)


def remote(src, dst, send, recv, rep, shard):
    return pltpu.make_async_remote_copy(
        src_ref=src, dst_ref=dst, send_sem=send, recv_sem=recv,
        device_id={"rep": rep, "shard": shard}, device_id_type=pl.DeviceIdType.MESH,
    )


def forward_kernel(
    pooled_ref, ids_ref, own_ids_ref, tables_ref, large_out, ids_out, small_out,
    send, recv, id_send, id_recv, own,
):
    copies, groups = lax.axis_size("rep"), lax.axis_size("shard")
    devices = copies * groups
    rep, me = lax.axis_index("rep"), lax.axis_index("shard")
    index = rep * groups + me

    def block(k):
        to = lax.rem(me + k, groups)
        return remote(pooled_ref.at[to], large_out.at[me], send.at[k], recv.at[k], rep, to)

    def ids(k):
        to = lax.rem(index + k, devices)
        return remote(
            ids_ref.at[to], ids_out.at[index], id_send.at[k], id_recv.at[k],
            to // groups, lax.rem(to, groups),
        )

    def block_in(k):
        at = lax.rem(me + groups - k, groups)
        return remote(pooled_ref.at[at], large_out.at[at], send.at[k], recv.at[k], rep, at)

    def ids_in(k):
        at = lax.rem(index + devices - k, devices)
        return remote(
            ids_ref.at[at], ids_out.at[at], id_send.at[k], id_recv.at[k],
            at // groups, lax.rem(at, groups),
        )

    def run(low, high, act):
        def body(k, c):
            act(k)
            return c

        lax.fori_loop(low, high, body, 0)

    greet_all()
    run(1, groups, lambda k: block(k).start())
    run(1, devices, lambda k: ids(k).start())
    mine = pltpu.make_async_copy(pooled_ref.at[me], large_out.at[me], own.at[0])
    mine_ids = pltpu.make_async_copy(ids_ref.at[index], ids_out.at[index], own.at[1])
    mine.start()
    mine_ids.start()
    batch, small_count = own_ids_ref.shape
    rows = iota((batch, tables_ref.shape[1]), 1)
    for t in range(small_count):
        hot = (own_ids_ref[:, t : t + 1] == rows).astype(f32).astype(bf16)
        small_out[t] = jnp.dot(hot, tables_ref[t], preferred_element_type=f32).astype(bf16)
    mine.wait()
    mine_ids.wait()
    run(1, groups, lambda k: block_in(k).wait_recv())
    run(1, devices, lambda k: ids_in(k).wait_recv())
    run(1, groups, lambda k: block(k).wait_send())
    run(1, devices, lambda k: ids(k).wait_send())


def forward(pooled, ids, own_ids, tables):
    groups, devices = pooled.shape[0], ids.shape[0]
    return pl.pallas_call(
        forward_kernel,
        out_shape=(
            jax.ShapeDtypeStruct(pooled.shape, pooled.dtype),
            jax.ShapeDtypeStruct(ids.shape, ids.dtype),
            jax.ShapeDtypeStruct(
                (tables.shape[0], own_ids.shape[0], tables.shape[2]), tables.dtype
            ),
        ),
        in_specs=[whole(pltpu.VMEM)] * 4,
        out_specs=(whole(pltpu.VMEM),) * 3,
        scratch_shapes=[pltpu.SemaphoreType.DMA((groups,))] * 2
        + [pltpu.SemaphoreType.DMA((devices,))] * 2
        + [pltpu.SemaphoreType.DMA((2,))],
        compiler_params=pltpu.CompilerParams(
            collective_id=0, has_side_effects=True, vmem_limit_bytes=VMEM_LIMIT
        ),
        name="forward",
    )(pooled, ids, own_ids, tables)


def fold_kernel(fold_ref, out_ref, send, recv, far_send, far_recv, own):
    copies, groups = lax.axis_size("rep"), lax.axis_size("shard")
    rep, me = lax.axis_index("rep"), lax.axis_index("shard")
    other = 1 - rep

    def out_block(k):
        to = lax.rem(me + k, groups)
        return remote(
            fold_ref.at[to], out_ref.at[rep * groups + me], send.at[k], recv.at[k], rep, to
        )

    def in_block(k):
        at = lax.rem(me + groups - k, groups)
        return remote(
            fold_ref.at[at], out_ref.at[rep * groups + at], send.at[k], recv.at[k], rep, at
        )

    def far_out(k):
        slot = out_ref.at[rep * groups + lax.rem(me + groups - k, groups)]
        return remote(slot, slot, far_send.at[k], far_recv.at[k], other, me)

    def far_in(k):
        slot = out_ref.at[other * groups + lax.rem(me + groups - k, groups)]
        return remote(slot, slot, far_send.at[k], far_recv.at[k], other, me)

    own_far = remote(
        fold_ref.at[me], out_ref.at[rep * groups + me], far_send.at[0], far_recv.at[0], other, me
    )

    def run(act):
        def body(k, c):
            act(k)
            return c

        lax.fori_loop(1, groups, body, 0)

    greet_all()
    run(lambda k: out_block(k).start())
    own_far.start()
    mine = pltpu.make_async_copy(fold_ref.at[me], out_ref.at[rep * groups + me], own.at[0])
    mine.start()

    def pass_on(k):
        in_block(k).wait_recv()
        far_out(k).start()

    run(pass_on)
    mine.wait()
    far_in(0).wait_recv()
    run(lambda k: far_in(k).wait_recv())
    own_far.wait_send()
    run(lambda k: far_out(k).wait_send())
    run(lambda k: out_block(k).wait_send())


def fold_exchange(fold, copies):
    groups = fold.shape[0]
    return pl.pallas_call(
        fold_kernel,
        out_shape=jax.ShapeDtypeStruct((copies * groups,) + fold.shape[1:], fold.dtype),
        in_specs=[whole(pltpu.VMEM)],
        out_specs=whole(pltpu.VMEM),
        scratch_shapes=[pltpu.SemaphoreType.DMA((groups,))] * 4 + [pltpu.SemaphoreType.DMA((1,))],
        compiler_params=pltpu.CompilerParams(
            collective_id=1, has_side_effects=True, vmem_limit_bytes=VMEM_LIMIT
        ),
        cost_estimate=pl.CostEstimate(
            flops=400 * fold.size * LANES, bytes_accessed=4 * fold.size, transcendentals=0
        ),
        name="fold_exchange",
    )(fold)


def spread_kernel(own_ref, out_ref, send_z, send_1, send_2, send_core, recv, local):
    groups = lax.axis_size("shard")
    ring = groups // 4
    rep, member = lax.axis_index("rep"), lax.axis_index("shard")
    z, y, core = member // 4, lax.rem(member, 4) // 2, lax.rem(member, 2)

    def shard_of(z_at, y_at, core_at):
        return z_at * 4 + y_at * 2 + core_at

    def send(h, src, rep_at, z_at, y_at, sem, to_rep, to_z, to_y, to_core):
        slot = rep_at * groups + shard_of(z_at, y_at, core)
        source = out_ref.at[slot, h] if src is None else src
        return remote(
            source, out_ref.at[slot, h], sem, recv.at[h, slot],
            to_rep, shard_of(to_z, to_y, to_core),
        )

    def arrived(h, rep_at, z_at, y_at, core_at):
        slot = rep_at * groups + shard_of(z_at, y_at, core_at)
        place = out_ref.at[slot, h]
        remote(place, place, local.at[1], recv.at[h, slot], rep, member).wait_recv()

    greet_all()
    pending = []

    def go(copy):
        copy.start()
        pending.append(copy)

    def second(h, k, src, rep_at, z_at, y_at):
        hop = (rep, z, 1 - y, core) if h == 0 else (1 - rep, z, y, core)
        go(send(h, src, rep_at, z_at, y_at, send_1.at[h, k], *hop))

    def third(h, k, src, rep_at, z_at, y_at):
        hop = (1 - rep, z, y, core) if h == 0 else (rep, z, 1 - y, core)
        go(send(h, src, rep_at, z_at, y_at, send_2.at[h, k], *hop))

    def last(h, k, src, rep_at, z_at, y_at):
        go(send(h, src, rep_at, z_at, y_at, send_core.at[h, k], rep, z, y, 1 - core))

    for k in range(1, ring):
        for h in range(2):
            go(send(h, own_ref.at[h], rep, z, y, send_z.at[h, k], rep, lax.rem(z + k, ring), y, core))
    for h in range(2):
        src = own_ref.at[h]
        second(h, 0, src, rep, z, y)
        third(h, 0, src, rep, z, y)
        last(h, 0, src, rep, z, y)
    mine = pltpu.make_async_copy(
        own_ref, out_ref.at[rep * groups + member], local.at[0]
    )
    mine.start()
    for k in range(1, ring):
        z_at = lax.rem(z + ring - k, ring)
        for h in range(2):
            arrived(h, rep, z_at, y, core)
            second(h, k, None, rep, z_at, y)
            third(h, k, None, rep, z_at, y)
            last(h, k, None, rep, z_at, y)
    for k in range(ring):
        z_at = lax.rem(z + ring - k, ring)
        for h in range(2):
            where = (rep, z_at, 1 - y) if h == 0 else (1 - rep, z_at, y)
            arrived(h, *where, core)
            third(h, ring + k, None, *where)
            last(h, ring + k, None, *where)
    for k in range(2 * ring):
        z_at = lax.rem(z + ring - k % ring, ring)
        for h in range(2):
            if h == 0:
                where = (1 - rep, z_at, y if k < ring else 1 - y)
            else:
                where = (rep if k < ring else 1 - rep, z_at, 1 - y)
            arrived(h, *where, core)
            last(h, 2 * ring + k, None, *where)
    for r in range(2):
        for k in range(ring):
            for y_at in range(2):
                for h in range(2):
                    arrived(h, r, k, y_at, 1 - core)
    mine.wait()
    for copy in pending:
        copy.wait_send()


def spread_all(own, copies, groups):
    rows, width = own.shape
    ring = groups // 4
    devices = copies * groups
    out = pl.pallas_call(
        spread_kernel,
        out_shape=jax.ShapeDtypeStruct((devices, 2, rows // 2, width), own.dtype),
        in_specs=[whole(pltpu.VMEM)],
        out_specs=whole(pltpu.VMEM),
        scratch_shapes=[
            pltpu.SemaphoreType.DMA((2, ring)),
            pltpu.SemaphoreType.DMA((2, ring)),
            pltpu.SemaphoreType.DMA((2, 2 * ring)),
            pltpu.SemaphoreType.DMA((2, 4 * ring)),
            pltpu.SemaphoreType.DMA((2, devices)),
            pltpu.SemaphoreType.DMA((2,)),
        ],
        compiler_params=pltpu.CompilerParams(
            collective_id=2, has_side_effects=True, vmem_limit_bytes=VMEM_LIMIT
        ),
        name="spread_all",
    )(own.reshape(2, rows // 2, width))
    return out.reshape(devices * rows, width)


def shards(
    dense, small_ids, labels, small_tables, large_tables, batch_sizes, bag_ends,
    owner_row_index, w_first, b_first, w_out,
):
    groups = lax.axis_size("shard")
    copies = lax.axis_size("rep")
    devices = groups * copies
    first = lax.axis_index("rep") * groups
    index = first + lax.axis_index("shard")
    small_count, small_rows, width = small_tables.shape
    per_table = devices // small_count
    ends, rows, table = bag_ends[0], owner_row_index[0], large_tables[0]

    sent_ids = jnp.repeat(jnp.transpose(small_ids), per_table, axis=0)[:, None]
    pooled = pool(first[None], groups, rows, ends, table)
    large, all_ids, small = forward(pooled, sent_ids, small_ids, small_tables)
    small_grads, fold = top(
        index[None], batch_sizes, dense, labels, small, large, w_first, b_first, w_out
    )
    fold_all = fold_exchange(fold, copies)
    sent = jnp.repeat(small_grads, per_table, axis=0)
    arrived = lax.all_to_all(sent, ("rep", "shard"), split_axis=0, concat_axis=0, tiled=True)
    large_new = scatter(rows, ends, fold_all, table)
    part_rows = small_count * small_rows // devices
    flat = small_tables.reshape(small_count * small_rows, width)
    own = lax.dynamic_slice_in_dim(flat, index * part_rows, part_rows, 0)
    first_row = (lax.rem(index, per_table) * part_rows)[None].astype(jnp.int32)
    updated = small_update(first_row, all_ids[:, 0], arrived, own)
    small_new = spread_all(updated, copies, groups).reshape(small_count, small_rows, width)
    return small_new, large_new[None]


def solution(mesh):
    both = ("rep", "shard")
    placed = (
        P(both, None), P(both, None), P(both), P(), P("shard", None, None), P(),
        P("shard", None, None), P("shard", None, None), P(), P(), P(),
    )
    return jax.shard_map(
        shards, mesh=mesh, in_specs=placed, out_specs=(P(), P("shard", None, None)), check_vma=False
    )
```

```python
import functools

import jax
import jax.numpy as jnp
from jax import lax
from jax.experimental import pallas as pl
from jax.experimental.pallas import tpu as pltpu
from jax.sharding import PartitionSpec as P

step_size = 32.0
LANES = 128
VMEM_LIMIT = 60 * 1024 * 1024
f32 = jnp.float32
bf16 = jnp.bfloat16


def whole(space):
    return pl.BlockSpec(memory_space=space)


def iota(shape, axis):
    return lax.broadcasted_iota(jnp.int32, shape, axis)


def members_of(ends, slots):
    span = ends.shape[-1]
    starts = jnp.where(iota((1, span), 1) == 0, 0, pltpu.roll(ends, 1, 1))
    places = iota((slots, span), 0)
    return ((places >= starts) & (places < ends)).astype(f32).astype(bf16)


def pool_kernel(first_ref, rows_ref, count_ref, ends_ref, table_ref, out_ref, wide, picked):
    slots = rows_ref.shape[1]
    owners = out_ref.shape[0]
    last = count_ref.shape[1] - 1
    first = first_ref[0]
    wide[...] = table_ref[...].astype(f32)
    picked[...] = jnp.zeros_like(picked)

    def owner(o, carry):
        d = o + first

        def group(g, c):
            base = pl.multiple_of(g * 8, 8)
            parts = [wide[pl.ds(rows_ref[d, base + u], 1), :] for u in range(8)]
            picked[pl.ds(pl.multiple_of(o * slots + base, 8), 8), :] = jnp.concatenate(parts, axis=0)
            return c

        return lax.fori_loop(0, (count_ref[d, last] + 7) // 8, group, carry)

    lax.fori_loop(0, owners, owner, 0)

    def sums(o, carry):
        members = members_of(ends_ref[pl.ds(o + first, 1), :], slots)
        block = picked[pl.ds(pl.multiple_of(o * slots, 8), slots), :].astype(bf16)
        pooled = lax.dot_general(
            members, block, (((0,), (0,)), ((), ())), preferred_element_type=f32
        )
        out_ref[o] = pooled.astype(bf16)
        return carry

    lax.fori_loop(0, owners, sums, 0, unroll=4)


def pool(first, owners, rows, ends, table):
    slots = rows.shape[1]
    width = table.shape[1]
    return pl.pallas_call(
        pool_kernel,
        out_shape=jax.ShapeDtypeStruct((owners, ends.shape[1], width), bf16),
        in_specs=[whole(pltpu.SMEM)] * 3 + [whole(pltpu.VMEM)] * 2,
        out_specs=whole(pltpu.VMEM),
        scratch_shapes=[
            pltpu.VMEM(table.shape, f32),
            pltpu.VMEM((owners * slots, width), f32),
        ],
        compiler_params=pltpu.CompilerParams(vmem_limit_bytes=VMEM_LIMIT),
        name="pool",
    )(first, rows, ends, ends, table)


def scatter_kernel(rows_ref, count_ref, ends_ref, fold_ref, table_ref, out_ref, spread, *sums):
    owners, slots = rows_ref.shape
    last = count_ref.shape[1] - 1
    lanes_of = len(sums)
    for total in sums:
        total[...] = jnp.zeros_like(total)

    def expand(d, carry):
        members = members_of(ends_ref[pl.ds(d, 1), :], slots)
        spread[pl.ds(pl.multiple_of(d * slots, 8), slots), :] = jnp.dot(
            members, fold_ref[d], preferred_element_type=f32
        )
        return carry

    lax.fori_loop(0, owners, expand, 0, unroll=4)

    def owner(d, carry):
        def group(g, c):
            base = pl.multiple_of(g * 8, 8)
            block = spread[pl.ds(pl.multiple_of(d * slots + base, 8), 8), :]
            for u in range(0, 8, lanes_of):
                spots = [rows_ref[d, base + u + v] for v in range(lanes_of)]
                news = [
                    sums[v][pl.ds(spots[v], 1), :] + block[u + v : u + v + 1]
                    for v in range(lanes_of)
                ]
                for v in range(lanes_of):
                    sums[v][pl.ds(spots[v], 1), :] = news[v]
            return c

        return lax.fori_loop(0, (count_ref[d, last] + 7) // 8, group, carry)

    lax.fori_loop(0, owners, owner, 0)
    step = 256

    def finish(g, c):
        at = pl.ds(pl.multiple_of(g * step, step), step)
        total = sums[0][at, :]
        for other in sums[1:]:
            total = total + other[at, :]
        out_ref[at, :] = (table_ref[at, :].astype(f32) - step_size * total).astype(bf16)
        return c

    lax.fori_loop(0, table_ref.shape[0] // step, finish, 0)


def scatter(rows, ends, fold, table):
    slots = rows.shape[1]
    return pl.pallas_call(
        scatter_kernel,
        out_shape=jax.ShapeDtypeStruct(table.shape, bf16),
        in_specs=[whole(pltpu.SMEM), whole(pltpu.SMEM)] + [whole(pltpu.VMEM)] * 3,
        out_specs=whole(pltpu.VMEM),
        scratch_shapes=[pltpu.VMEM((rows.size, table.shape[1]), f32)]
        + [pltpu.VMEM(table.shape, f32)] * 4,
        compiler_params=pltpu.CompilerParams(vmem_limit_bytes=VMEM_LIMIT),
        cost_estimate=pl.CostEstimate(
            flops=20 * table.size * LANES, bytes_accessed=4 * table.size, transcendentals=0
        ),
        name="scatter",
    )(rows, ends, ends, fold, table)


def small_kernel(part_rows, first_ref, ids_ref, grads_ref, table_ref, out_ref):
    senders, batch = ids_ref.shape
    rows = iota((part_rows, batch), 0) + first_ref[0]
    total = jnp.zeros(out_ref.shape, f32)

    def one(s, total):
        hot = (rows == ids_ref[pl.ds(s, 1), :]).astype(f32).astype(bf16)
        return total + jnp.dot(hot, grads_ref[s], preferred_element_type=f32)

    total = lax.fori_loop(0, senders, one, total, unroll=8)
    out_ref[...] = (table_ref[...].astype(f32) - step_size * total).astype(bf16)


def small_update(first, ids, grads, rows):
    return pl.pallas_call(
        functools.partial(small_kernel, rows.shape[0]),
        out_shape=jax.ShapeDtypeStruct(rows.shape, bf16),
        in_specs=[whole(pltpu.SMEM)] + [whole(pltpu.VMEM)] * 3,
        out_specs=whole(pltpu.VMEM),
        compiler_params=pltpu.CompilerParams(vmem_limit_bytes=VMEM_LIMIT),
        name="small_update",
    )(first, ids, grads, rows)


def spans_of(vec_count):
    return [(i, i * (i - 1) // 2) for i in range(1, vec_count)]


def top_kernel(
    vec_count, pad, index_ref, sizes_ref, dense_ref, labels_ref, small_ref, large_ref,
    w_ref, bias_ref, wout_ref, small_out, fold_out, vecs, gram, pairs, spread,
):
    batch, width = dense_ref.shape
    small_count = small_ref.shape[0]
    feats, bag_span = large_ref.shape[0], large_ref.shape[1]
    pair_pad = pairs.shape[1]
    pair_count = vec_count * (vec_count - 1) // 2
    scale = width ** (-0.5)
    spans = spans_of(vec_count)

    def rows_of(i):
        return pl.ds(i, batch, stride=pad)

    vecs[rows_of(0), :] = dense_ref[...].astype(f32)
    for t in range(small_count):
        vecs[rows_of(1 + t), :] = small_ref[t].astype(f32)
    sample = iota((batch, bag_span), 0)
    bag = iota((batch, bag_span), 1) * batch
    for f in range(feats):
        reach = sample * sizes_ref[f, index_ref[0]]
        hot = ((reach >= bag) & (reach < bag + batch)).astype(f32).astype(bf16)
        vecs[rows_of(1 + small_count + f), :] = jnp.dot(
            hot, large_ref[f], preferred_element_type=f32
        )
    for i in range(vec_count, pad):
        vecs[rows_of(i), :] = jnp.zeros((batch, width), f32)

    unroll = 8

    def gram_step(g, c):
        for u in range(unroll):
            at = pl.ds(pl.multiple_of((g * unroll + u) * pad, 8), pad)
            own = vecs[at, :].astype(bf16)
            gram[at, 0:pad] = lax.dot_general(
                own, own, (((1,), (1,)), ((), ())), preferred_element_type=f32
            )
        return c

    lax.fori_loop(0, batch // unroll, gram_step, 0)

    lane = iota((1, LANES), 1)
    chunk = 64
    for start in range(0, batch, chunk):
        tile = jnp.zeros((chunk, LANES), f32)
        at_tile = 0
        for i, off in spans:
            piece = gram[pl.ds(start * pad + i, chunk, stride=pad), :]
            turn = off % LANES
            if turn:
                piece = pltpu.roll(piece, turn, 1)
            low = off - at_tile * LANES
            tile = jnp.where((lane >= low) & (lane < low + i), piece, tile)
            if low + i >= LANES:
                pairs[start : start + chunk, at_tile * LANES : (at_tile + 1) * LANES] = (
                    tile * scale
                ).astype(bf16)
                at_tile += 1
                rest = low + i - LANES
                tile = jnp.where(lane < rest, piece, jnp.zeros_like(piece))
        if at_tile * LANES < pair_pad:
            pairs[start : start + chunk, at_tile * LANES : pair_pad] = (tile * scale).astype(bf16)

    block = 128
    labels_col = jnp.transpose(
        jnp.broadcast_to(labels_ref[...].astype(f32), (LANES, batch))
    )[:, 0:1]
    for start in range(0, batch, block):
        at = slice(start, start + block)
        preact = (
            jnp.dot(pairs[at, :], w_ref[0:pair_pad, :], preferred_element_type=f32)
            + jnp.dot(dense_ref[at, :], w_ref[pair_count : pair_count + width, :], preferred_element_type=f32)
            + bias_ref[...]
        )
        squash = jax.nn.sigmoid(preact)
        logits = jnp.sum(preact * squash * wout_ref[...], axis=1, keepdims=True)
        grad = jax.nn.sigmoid(logits) - labels_col[at, :]
        pre_grad = (
            grad * wout_ref[...] * (squash * (1.0 + preact * (1.0 - squash)))
        ).astype(bf16)
        for q in range(0, pair_pad, LANES):
            spread[at, q : q + LANES] = lax.dot_general(
                pre_grad, w_ref[q : q + LANES, :], (((1,), (1,)), ((), ())),
                preferred_element_type=f32,
            ) * scale

    gram[rows_of(0), :] = jnp.zeros((batch, LANES), f32)
    for i in range(vec_count, pad):
        gram[rows_of(i), :] = jnp.zeros((batch, LANES), f32)
    for start in range(0, batch, chunk):
        for i, off in spans:
            first = off // LANES
            low = off - first * LANES
            here = spread[start : start + chunk, first * LANES : (first + 1) * LANES]
            if low + i > LANES:
                after = spread[start : start + chunk, (first + 1) * LANES : (first + 2) * LANES]
                here = jnp.where(lane >= low, here, after)
            if low:
                here = pltpu.roll(here, LANES - low, 1)
            gram[pl.ds(start * pad + i, chunk, stride=pad), :] = jnp.where(lane < i, here, 0.0)

    def back_step(g, c):
        for u in range(unroll):
            at = pl.ds(pl.multiple_of((g * unroll + u) * pad, 8), pad)
            lower = gram[at, :]
            both = lower[:, 0:pad] + jnp.transpose(lower)[0:pad, :]
            vecs[at, :] = jnp.dot(
                both.astype(bf16), vecs[at, :].astype(bf16), preferred_element_type=f32
            )
        return c

    lax.fori_loop(0, batch // unroll, back_step, 0)

    for t in range(small_count):
        small_out[t] = vecs[rows_of(1 + t), :].astype(bf16)
    sample_lane = iota((bag_span, batch), 1)
    bag_row = iota((bag_span, batch), 0) * batch
    for f in range(feats):
        reach = sample_lane * sizes_ref[f, index_ref[0]]
        hot = ((reach >= bag_row) & (reach < bag_row + batch)).astype(f32).astype(bf16)
        fold_out[f] = jnp.dot(
            hot, vecs[rows_of(1 + small_count + f), :].astype(bf16), preferred_element_type=f32
        ).astype(bf16)


def top(index, sizes, dense, labels, small, large, w_first, bias, wout):
    batch, width = dense.shape
    small_count, feats, bag_span = small.shape[0], large.shape[0], large.shape[1]
    vec_count = 1 + small_count + feats
    pad = -(-vec_count // 8) * 8
    pair_count = vec_count * (vec_count - 1) // 2
    pair_pad = -(-pair_count // LANES) * LANES
    return pl.pallas_call(
        functools.partial(top_kernel, vec_count, pad),
        out_shape=(
            jax.ShapeDtypeStruct((small_count, batch, width), bf16),
            jax.ShapeDtypeStruct((feats, bag_span, width), bf16),
        ),
        in_specs=[whole(pltpu.SMEM)] * 2 + [whole(pltpu.VMEM)] * 7,
        out_specs=(whole(pltpu.VMEM), whole(pltpu.VMEM)),
        scratch_shapes=[
            pltpu.VMEM((batch * pad, width), f32),
            pltpu.VMEM((batch * pad, LANES), f32),
            pltpu.VMEM((batch, pair_pad), bf16),
            pltpu.VMEM((batch, pair_pad), f32),
        ],
        compiler_params=pltpu.CompilerParams(vmem_limit_bytes=VMEM_LIMIT),
        name="top",
    )(
        index, sizes, dense, labels[None, :], small, large, w_first,
        bias[None, :], wout[None, :],
    )


def greet_all():
    copies, groups = lax.axis_size("rep"), lax.axis_size("shard")
    devices = copies * groups
    index = lax.axis_index("rep") * groups + lax.axis_index("shard")
    barrier = pltpu.get_barrier_semaphore()

    def greet(k, c):
        other = lax.rem(index + k, devices)
        pl.semaphore_signal(
            barrier, inc=1, device_id={"rep": other // groups, "shard": lax.rem(other, groups)},
            device_id_type=pl.DeviceIdType.MESH,
        )
        return c

    lax.fori_loop(1, devices, greet, 0)
    pl.semaphore_wait(barrier, devices - 1)


def remote(src, dst, send, recv, rep, shard):
    return pltpu.make_async_remote_copy(
        src_ref=src, dst_ref=dst, send_sem=send, recv_sem=recv,
        device_id={"rep": rep, "shard": shard}, device_id_type=pl.DeviceIdType.MESH,
    )


def forward_kernel(
    pooled_ref, ids_ref, own_ids_ref, tables_ref, large_out, ids_out, small_out,
    send, recv, id_send, id_recv, own, tables,
):
    copies, groups = lax.axis_size("rep"), lax.axis_size("shard")
    devices = copies * groups
    rep, me = lax.axis_index("rep"), lax.axis_index("shard")
    index = rep * groups + me

    def block(k):
        to = lax.rem(me + k, groups)
        return remote(pooled_ref.at[to], large_out.at[me], send.at[k], recv.at[k], rep, to)

    def ids(k):
        to = lax.rem(index + k, devices)
        return remote(
            ids_ref.at[to], ids_out.at[index], id_send.at[k], id_recv.at[k],
            to // groups, lax.rem(to, groups),
        )

    def block_in(k):
        at = lax.rem(me + groups - k, groups)
        return remote(pooled_ref.at[at], large_out.at[at], send.at[k], recv.at[k], rep, at)

    def ids_in(k):
        at = lax.rem(index + devices - k, devices)
        return remote(
            ids_ref.at[at], ids_out.at[at], id_send.at[k], id_recv.at[k],
            at // groups, lax.rem(at, groups),
        )

    def run(low, high, act):
        def body(k, c):
            act(k)
            return c

        lax.fori_loop(low, high, body, 0)

    fetch = pltpu.make_async_copy(tables_ref, tables, own.at[2])
    fetch.start()
    greet_all()
    run(1, groups, lambda k: block(k).start())
    run(1, devices, lambda k: ids(k).start())
    mine = pltpu.make_async_copy(pooled_ref.at[me], large_out.at[me], own.at[0])
    mine_ids = pltpu.make_async_copy(ids_ref.at[index], ids_out.at[index], own.at[1])
    mine.start()
    mine_ids.start()
    batch, small_count = own_ids_ref.shape
    rows = iota((batch, tables_ref.shape[1]), 1)
    fetch.wait()
    for t in range(small_count):
        hot = (own_ids_ref[:, t : t + 1] == rows).astype(f32).astype(bf16)
        small_out[t] = jnp.dot(hot, tables[t], preferred_element_type=f32).astype(bf16)
    mine.wait()
    mine_ids.wait()
    run(1, groups, lambda k: block_in(k).wait_recv())
    run(1, devices, lambda k: ids_in(k).wait_recv())
    run(1, groups, lambda k: block(k).wait_send())
    run(1, devices, lambda k: ids(k).wait_send())


def forward(pooled, ids, own_ids, tables):
    groups, devices = pooled.shape[0], ids.shape[0]
    return pl.pallas_call(
        forward_kernel,
        out_shape=(
            jax.ShapeDtypeStruct(pooled.shape, pooled.dtype),
            jax.ShapeDtypeStruct(ids.shape, ids.dtype),
            jax.ShapeDtypeStruct(
                (tables.shape[0], own_ids.shape[0], tables.shape[2]), tables.dtype
            ),
        ),
        in_specs=[whole(pltpu.VMEM)] * 3 + [whole(pl.ANY)],
        out_specs=(whole(pltpu.VMEM),) * 3,
        scratch_shapes=[pltpu.SemaphoreType.DMA((groups,))] * 2
        + [pltpu.SemaphoreType.DMA((devices,))] * 2
        + [pltpu.SemaphoreType.DMA((3,)), pltpu.VMEM(tables.shape, tables.dtype)],
        compiler_params=pltpu.CompilerParams(
            collective_id=0, has_side_effects=True, vmem_limit_bytes=VMEM_LIMIT
        ),
        name="forward",
    )(pooled, ids, own_ids, tables)


def fold_kernel(fold_ref, out_ref, send, recv, far_send, far_recv, own):
    copies, groups = lax.axis_size("rep"), lax.axis_size("shard")
    rep, me = lax.axis_index("rep"), lax.axis_index("shard")
    other = 1 - rep

    def out_block(k):
        to = lax.rem(me + k, groups)
        return remote(
            fold_ref.at[to], out_ref.at[rep * groups + me], send.at[k], recv.at[k], rep, to
        )

    def in_block(k):
        at = lax.rem(me + groups - k, groups)
        return remote(
            fold_ref.at[at], out_ref.at[rep * groups + at], send.at[k], recv.at[k], rep, at
        )

    def far_out(k):
        slot = out_ref.at[rep * groups + lax.rem(me + groups - k, groups)]
        return remote(slot, slot, far_send.at[k], far_recv.at[k], other, me)

    def far_in(k):
        slot = out_ref.at[other * groups + lax.rem(me + groups - k, groups)]
        return remote(slot, slot, far_send.at[k], far_recv.at[k], other, me)

    own_far = remote(
        fold_ref.at[me], out_ref.at[rep * groups + me], far_send.at[0], far_recv.at[0], other, me
    )

    def run(act):
        def body(k, c):
            act(k)
            return c

        lax.fori_loop(1, groups, body, 0)

    greet_all()
    run(lambda k: out_block(k).start())
    own_far.start()
    mine = pltpu.make_async_copy(fold_ref.at[me], out_ref.at[rep * groups + me], own.at[0])
    mine.start()

    def pass_on(k):
        in_block(k).wait_recv()
        far_out(k).start()

    run(pass_on)
    mine.wait()
    far_in(0).wait_recv()
    run(lambda k: far_in(k).wait_recv())
    own_far.wait_send()
    run(lambda k: far_out(k).wait_send())
    run(lambda k: out_block(k).wait_send())


def fold_exchange(fold, copies):
    groups = fold.shape[0]
    return pl.pallas_call(
        fold_kernel,
        out_shape=jax.ShapeDtypeStruct((copies * groups,) + fold.shape[1:], fold.dtype),
        in_specs=[whole(pltpu.VMEM)],
        out_specs=whole(pltpu.VMEM),
        scratch_shapes=[pltpu.SemaphoreType.DMA((groups,))] * 4 + [pltpu.SemaphoreType.DMA((1,))],
        compiler_params=pltpu.CompilerParams(
            collective_id=1, has_side_effects=True, vmem_limit_bytes=VMEM_LIMIT
        ),
        cost_estimate=pl.CostEstimate(
            flops=400 * fold.size * LANES, bytes_accessed=4 * fold.size, transcendentals=0
        ),
        name="fold_exchange",
    )(fold)


def spread_kernel(own_ref, out_ref, send_z, send_1, send_2, send_core, recv, local):
    groups = lax.axis_size("shard")
    ring = groups // 4
    rep, member = lax.axis_index("rep"), lax.axis_index("shard")
    z, y, core = member // 4, lax.rem(member, 4) // 2, lax.rem(member, 2)

    def shard_of(z_at, y_at, core_at):
        return z_at * 4 + y_at * 2 + core_at

    def send(h, src, rep_at, z_at, y_at, sem, to_rep, to_z, to_y, to_core):
        slot = rep_at * groups + shard_of(z_at, y_at, core)
        source = out_ref.at[slot, h] if src is None else src
        return remote(
            source, out_ref.at[slot, h], sem, recv.at[h, slot],
            to_rep, shard_of(to_z, to_y, to_core),
        )

    def arrived(h, rep_at, z_at, y_at, core_at):
        slot = rep_at * groups + shard_of(z_at, y_at, core_at)
        place = out_ref.at[slot, h]
        remote(place, place, local.at[1], recv.at[h, slot], rep, member).wait_recv()

    greet_all()
    pending = []

    def go(copy):
        copy.start()
        pending.append(copy)

    def second(h, k, src, rep_at, z_at, y_at):
        hop = (rep, z, 1 - y, core) if h == 0 else (1 - rep, z, y, core)
        go(send(h, src, rep_at, z_at, y_at, send_1.at[h, k], *hop))

    def third(h, k, src, rep_at, z_at, y_at):
        hop = (1 - rep, z, y, core) if h == 0 else (rep, z, 1 - y, core)
        go(send(h, src, rep_at, z_at, y_at, send_2.at[h, k], *hop))

    def last(h, k, src, rep_at, z_at, y_at):
        go(send(h, src, rep_at, z_at, y_at, send_core.at[h, k], rep, z, y, 1 - core))

    for k in range(1, ring):
        for h in range(2):
            go(send(h, own_ref.at[h], rep, z, y, send_z.at[h, k], rep, lax.rem(z + k, ring), y, core))
    for h in range(2):
        src = own_ref.at[h]
        second(h, 0, src, rep, z, y)
        third(h, 0, src, rep, z, y)
        last(h, 0, src, rep, z, y)
    mine = pltpu.make_async_copy(
        own_ref, out_ref.at[rep * groups + member], local.at[0]
    )
    mine.start()
    for k in range(1, ring):
        z_at = lax.rem(z + ring - k, ring)
        for h in range(2):
            arrived(h, rep, z_at, y, core)
            second(h, k, None, rep, z_at, y)
            third(h, k, None, rep, z_at, y)
            last(h, k, None, rep, z_at, y)
    for k in range(ring):
        z_at = lax.rem(z + ring - k, ring)
        for h in range(2):
            where = (rep, z_at, 1 - y) if h == 0 else (1 - rep, z_at, y)
            arrived(h, *where, core)
            third(h, ring + k, None, *where)
            last(h, ring + k, None, *where)
    for k in range(2 * ring):
        z_at = lax.rem(z + ring - k % ring, ring)
        for h in range(2):
            if h == 0:
                where = (1 - rep, z_at, y if k < ring else 1 - y)
            else:
                where = (rep if k < ring else 1 - rep, z_at, 1 - y)
            arrived(h, *where, core)
            last(h, 2 * ring + k, None, *where)
    for r in range(2):
        for k in range(ring):
            for y_at in range(2):
                for h in range(2):
                    arrived(h, r, k, y_at, 1 - core)
    mine.wait()
    for copy in pending:
        copy.wait_send()


def spread_all(own, copies, groups):
    rows, width = own.shape
    ring = groups // 4
    devices = copies * groups
    out = pl.pallas_call(
        spread_kernel,
        out_shape=jax.ShapeDtypeStruct((devices, 2, rows // 2, width), own.dtype),
        in_specs=[whole(pltpu.VMEM)],
        out_specs=whole(pltpu.VMEM),
        scratch_shapes=[
            pltpu.SemaphoreType.DMA((2, ring)),
            pltpu.SemaphoreType.DMA((2, ring)),
            pltpu.SemaphoreType.DMA((2, 2 * ring)),
            pltpu.SemaphoreType.DMA((2, 4 * ring)),
            pltpu.SemaphoreType.DMA((2, devices)),
            pltpu.SemaphoreType.DMA((2,)),
        ],
        compiler_params=pltpu.CompilerParams(
            collective_id=2, has_side_effects=True, vmem_limit_bytes=VMEM_LIMIT
        ),
        name="spread_all",
    )(own.reshape(2, rows // 2, width))
    return out.reshape(devices * rows, width)


def shards(
    dense, small_ids, labels, small_tables, large_tables, batch_sizes, bag_ends,
    owner_row_index, w_first, b_first, w_out,
):
    groups = lax.axis_size("shard")
    copies = lax.axis_size("rep")
    devices = groups * copies
    first = lax.axis_index("rep") * groups
    index = first + lax.axis_index("shard")
    small_count, small_rows, width = small_tables.shape
    per_table = devices // small_count
    ends, rows, table = bag_ends[0], owner_row_index[0], large_tables[0]

    sent_ids = jnp.repeat(jnp.transpose(small_ids), per_table, axis=0)[:, None]
    pooled = pool(first[None], groups, rows, ends, table)
    large, all_ids, small = forward(pooled, sent_ids, small_ids, small_tables)
    small_grads, fold = top(
        index[None], batch_sizes, dense, labels, small, large, w_first, b_first, w_out
    )
    fold_all = fold_exchange(fold, copies)
    sent = jnp.repeat(small_grads, per_table, axis=0)
    sent, fold_all = lax.optimization_barrier((sent, fold_all))
    arrived = lax.all_to_all(sent, ("rep", "shard"), split_axis=0, concat_axis=0, tiled=True)
    large_new = scatter(rows, ends, fold_all, table)
    part_rows = small_count * small_rows // devices
    flat = small_tables.reshape(small_count * small_rows, width)
    own = lax.dynamic_slice_in_dim(flat, index * part_rows, part_rows, 0)
    first_row = (lax.rem(index, per_table) * part_rows)[None].astype(jnp.int32)
    updated = small_update(first_row, all_ids[:, 0], arrived, own)
    small_new = spread_all(updated, copies, groups).reshape(small_count, small_rows, width)
    return small_new, large_new[None]


def solution(mesh):
    both = ("rep", "shard")
    placed = (
        P(both, None), P(both, None), P(both), P(), P("shard", None, None), P(),
        P("shard", None, None), P("shard", None, None), P(), P(), P(),
    )
    return jax.shard_map(
        shards, mesh=mesh, in_specs=placed, out_specs=(P(), P("shard", None, None)), check_vma=False
    )
```

```python
import functools

import jax
import jax.numpy as jnp
from jax import lax
from jax.experimental import pallas as pl
from jax.experimental.pallas import tpu as pltpu
from jax.sharding import PartitionSpec as P

step_size = 32.0
LANES = 128
VMEM_LIMIT = 60 * 1024 * 1024
f32 = jnp.float32
bf16 = jnp.bfloat16


def whole(space):
    return pl.BlockSpec(memory_space=space)


def iota(shape, axis):
    return lax.broadcasted_iota(jnp.int32, shape, axis)


def members_of(ends, slots):
    span = ends.shape[-1]
    starts = jnp.where(iota((1, span), 1) == 0, 0, pltpu.roll(ends, 1, 1))
    places = iota((slots, span), 0)
    return ((places >= starts) & (places < ends)).astype(f32).astype(bf16)


def pool_kernel(
    first_ref, rows_ref, count_ref, ends_ref, table_ref, ids_ref, out_ref, by_table, by_sample,
    wide, picked,
):
    by_sample[...] = jnp.transpose(ids_ref[...])
    per_table = by_table.shape[0] // ids_ref.shape[0]
    for n in range(by_table.shape[0]):
        t = n // per_table
        by_table[n] = ids_ref[t : t + 1, :]
    slots = rows_ref.shape[1]
    owners = out_ref.shape[0]
    last = count_ref.shape[1] - 1
    first = first_ref[0]
    wide[...] = table_ref[...].astype(f32)
    picked[...] = jnp.zeros_like(picked)

    def owner(o, carry):
        d = o + first

        def group(g, c):
            base = pl.multiple_of(g * 8, 8)
            parts = [wide[pl.ds(rows_ref[d, base + u], 1), :] for u in range(8)]
            picked[pl.ds(pl.multiple_of(o * slots + base, 8), 8), :] = jnp.concatenate(parts, axis=0)
            return c

        return lax.fori_loop(0, (count_ref[d, last] + 7) // 8, group, carry)

    lax.fori_loop(0, owners, owner, 0)

    def sums(o, carry):
        members = members_of(ends_ref[pl.ds(o + first, 1), :], slots)
        block = picked[pl.ds(pl.multiple_of(o * slots, 8), slots), :].astype(bf16)
        pooled = lax.dot_general(
            members, block, (((0,), (0,)), ((), ())), preferred_element_type=f32
        )
        out_ref[o] = pooled.astype(bf16)
        return carry

    lax.fori_loop(0, owners, sums, 0, unroll=4)


def pool(first, owners, rows, ends, table, ids, devices):
    slots = rows.shape[1]
    width = table.shape[1]
    return pl.pallas_call(
        pool_kernel,
        out_shape=(
            jax.ShapeDtypeStruct((owners, ends.shape[1], width), bf16),
            jax.ShapeDtypeStruct((devices, 1, ids.shape[1]), ids.dtype),
            jax.ShapeDtypeStruct((ids.shape[1], ids.shape[0]), ids.dtype),
        ),
        in_specs=[whole(pltpu.SMEM)] * 3 + [whole(pltpu.VMEM)] * 3,
        out_specs=(whole(pltpu.VMEM),) * 3,
        scratch_shapes=[
            pltpu.VMEM(table.shape, f32),
            pltpu.VMEM((owners * slots, width), f32),
        ],
        compiler_params=pltpu.CompilerParams(vmem_limit_bytes=VMEM_LIMIT),
        name="pool",
    )(first, rows, ends, ends, table, ids)


def scatter_kernel(rows_ref, count_ref, ends_ref, fold_ref, table_ref, out_ref, spread, *sums):
    owners, slots = rows_ref.shape
    last = count_ref.shape[1] - 1
    lanes_of = len(sums)
    for total in sums:
        total[...] = jnp.zeros_like(total)

    def expand(d, carry):
        members = members_of(ends_ref[pl.ds(d, 1), :], slots)
        spread[pl.ds(pl.multiple_of(d * slots, 8), slots), :] = jnp.dot(
            members, fold_ref[d], preferred_element_type=f32
        )
        return carry

    lax.fori_loop(0, owners, expand, 0, unroll=4)

    def owner(d, carry):
        def group(g, c):
            base = pl.multiple_of(g * 8, 8)
            block = spread[pl.ds(pl.multiple_of(d * slots + base, 8), 8), :]
            for u in range(0, 8, lanes_of):
                spots = [rows_ref[d, base + u + v] for v in range(lanes_of)]
                news = [
                    sums[v][pl.ds(spots[v], 1), :] + block[u + v : u + v + 1]
                    for v in range(lanes_of)
                ]
                for v in range(lanes_of):
                    sums[v][pl.ds(spots[v], 1), :] = news[v]
            return c

        return lax.fori_loop(0, (count_ref[d, last] + 7) // 8, group, carry)

    lax.fori_loop(0, owners, owner, 0)
    step = 256

    def finish(g, c):
        at = pl.ds(pl.multiple_of(g * step, step), step)
        total = sums[0][at, :]
        for other in sums[1:]:
            total = total + other[at, :]
        out_ref[at, :] = (table_ref[at, :].astype(f32) - step_size * total).astype(bf16)
        return c

    lax.fori_loop(0, table_ref.shape[0] // step, finish, 0)


def scatter(rows, ends, fold, table):
    slots = rows.shape[1]
    return pl.pallas_call(
        scatter_kernel,
        out_shape=jax.ShapeDtypeStruct(table.shape, bf16),
        in_specs=[whole(pltpu.SMEM), whole(pltpu.SMEM)] + [whole(pltpu.VMEM)] * 3,
        out_specs=whole(pltpu.VMEM),
        scratch_shapes=[pltpu.VMEM((rows.size, table.shape[1]), f32)]
        + [pltpu.VMEM(table.shape, f32)] * 4,
        compiler_params=pltpu.CompilerParams(vmem_limit_bytes=VMEM_LIMIT),
        cost_estimate=pl.CostEstimate(
            flops=20 * table.size * LANES, bytes_accessed=4 * table.size, transcendentals=0
        ),
        name="scatter",
    )(rows, ends, ends, fold, table)


def small_kernel(part_rows, first_ref, ids_ref, grads_ref, table_ref, out_ref):
    senders, batch = ids_ref.shape
    rows = iota((part_rows, batch), 0) + first_ref[0]
    total = jnp.zeros(out_ref.shape, f32)

    def one(s, total):
        hot = (rows == ids_ref[pl.ds(s, 1), :]).astype(f32).astype(bf16)
        return total + jnp.dot(hot, grads_ref[s], preferred_element_type=f32)

    total = lax.fori_loop(0, senders, one, total, unroll=8)
    out_ref[...] = (table_ref[...].astype(f32) - step_size * total).astype(bf16)


def small_update(first, ids, grads, rows):
    return pl.pallas_call(
        functools.partial(small_kernel, rows.shape[0]),
        out_shape=jax.ShapeDtypeStruct(rows.shape, bf16),
        in_specs=[whole(pltpu.SMEM)] + [whole(pltpu.VMEM)] * 3,
        out_specs=whole(pltpu.VMEM),
        compiler_params=pltpu.CompilerParams(vmem_limit_bytes=VMEM_LIMIT),
        name="small_update",
    )(first, ids, grads, rows)


def spans_of(vec_count):
    return [(i, i * (i - 1) // 2) for i in range(1, vec_count)]


def top_kernel(
    vec_count, pad, index_ref, sizes_ref, dense_ref, labels_ref, small_ref, large_ref,
    w_ref, bias_ref, wout_ref, small_out, fold_out, vecs, gram, pairs, spread,
):
    batch, width = dense_ref.shape
    small_count = small_ref.shape[0]
    feats, bag_span = large_ref.shape[0], large_ref.shape[1]
    pair_pad = pairs.shape[1]
    pair_count = vec_count * (vec_count - 1) // 2
    scale = width ** (-0.5)
    spans = spans_of(vec_count)

    def rows_of(i):
        return pl.ds(i, batch, stride=pad)

    vecs[rows_of(0), :] = dense_ref[...].astype(f32)
    for t in range(small_count):
        vecs[rows_of(1 + t), :] = small_ref[t].astype(f32)
    sample = iota((batch, bag_span), 0)
    bag = iota((batch, bag_span), 1) * batch
    for f in range(feats):
        reach = sample * sizes_ref[f, index_ref[0]]
        hot = ((reach >= bag) & (reach < bag + batch)).astype(f32).astype(bf16)
        vecs[rows_of(1 + small_count + f), :] = jnp.dot(
            hot, large_ref[f], preferred_element_type=f32
        )
    for i in range(vec_count, pad):
        vecs[rows_of(i), :] = jnp.zeros((batch, width), f32)

    unroll = 8

    def gram_step(g, c):
        for u in range(unroll):
            at = pl.ds(pl.multiple_of((g * unroll + u) * pad, 8), pad)
            own = vecs[at, :].astype(bf16)
            gram[at, 0:pad] = lax.dot_general(
                own, own, (((1,), (1,)), ((), ())), preferred_element_type=f32
            )
        return c

    lax.fori_loop(0, batch // unroll, gram_step, 0)

    lane = iota((1, LANES), 1)
    chunk = 64
    for start in range(0, batch, chunk):
        tile = jnp.zeros((chunk, LANES), f32)
        at_tile = 0
        for i, off in spans:
            piece = gram[pl.ds(start * pad + i, chunk, stride=pad), :]
            turn = off % LANES
            if turn:
                piece = pltpu.roll(piece, turn, 1)
            low = off - at_tile * LANES
            tile = jnp.where((lane >= low) & (lane < low + i), piece, tile)
            if low + i >= LANES:
                pairs[start : start + chunk, at_tile * LANES : (at_tile + 1) * LANES] = (
                    tile * scale
                ).astype(bf16)
                at_tile += 1
                rest = low + i - LANES
                tile = jnp.where(lane < rest, piece, jnp.zeros_like(piece))
        if at_tile * LANES < pair_pad:
            pairs[start : start + chunk, at_tile * LANES : pair_pad] = (tile * scale).astype(bf16)

    block = 128
    labels_col = jnp.transpose(
        jnp.broadcast_to(labels_ref[...].astype(f32), (LANES, batch))
    )[:, 0:1]
    for start in range(0, batch, block):
        at = slice(start, start + block)
        preact = (
            jnp.dot(pairs[at, :], w_ref[0:pair_pad, :], preferred_element_type=f32)
            + jnp.dot(dense_ref[at, :], w_ref[pair_count : pair_count + width, :], preferred_element_type=f32)
            + bias_ref[...]
        )
        squash = jax.nn.sigmoid(preact)
        logits = jnp.sum(preact * squash * wout_ref[...], axis=1, keepdims=True)
        grad = jax.nn.sigmoid(logits) - labels_col[at, :]
        pre_grad = (
            grad * wout_ref[...] * (squash * (1.0 + preact * (1.0 - squash)))
        ).astype(bf16)
        for q in range(0, pair_pad, LANES):
            spread[at, q : q + LANES] = lax.dot_general(
                pre_grad, w_ref[q : q + LANES, :], (((1,), (1,)), ((), ())),
                preferred_element_type=f32,
            ) * scale

    gram[rows_of(0), :] = jnp.zeros((batch, LANES), f32)
    for i in range(vec_count, pad):
        gram[rows_of(i), :] = jnp.zeros((batch, LANES), f32)
    for start in range(0, batch, chunk):
        for i, off in spans:
            first = off // LANES
            low = off - first * LANES
            here = spread[start : start + chunk, first * LANES : (first + 1) * LANES]
            if low + i > LANES:
                after = spread[start : start + chunk, (first + 1) * LANES : (first + 2) * LANES]
                here = jnp.where(lane >= low, here, after)
            if low:
                here = pltpu.roll(here, LANES - low, 1)
            gram[pl.ds(start * pad + i, chunk, stride=pad), :] = jnp.where(lane < i, here, 0.0)

    def back_step(g, c):
        for u in range(unroll):
            at = pl.ds(pl.multiple_of((g * unroll + u) * pad, 8), pad)
            lower = gram[at, :]
            both = lower[:, 0:pad] + jnp.transpose(lower)[0:pad, :]
            vecs[at, :] = jnp.dot(
                both.astype(bf16), vecs[at, :].astype(bf16), preferred_element_type=f32
            )
        return c

    lax.fori_loop(0, batch // unroll, back_step, 0)

    for t in range(small_count):
        small_out[t] = vecs[rows_of(1 + t), :].astype(bf16)
    sample_lane = iota((bag_span, batch), 1)
    bag_row = iota((bag_span, batch), 0) * batch
    for f in range(feats):
        reach = sample_lane * sizes_ref[f, index_ref[0]]
        hot = ((reach >= bag_row) & (reach < bag_row + batch)).astype(f32).astype(bf16)
        fold_out[f] = jnp.dot(
            hot, vecs[rows_of(1 + small_count + f), :].astype(bf16), preferred_element_type=f32
        ).astype(bf16)


def top(index, sizes, dense, labels, small, large, w_first, bias, wout):
    batch, width = dense.shape
    small_count, feats, bag_span = small.shape[0], large.shape[0], large.shape[1]
    vec_count = 1 + small_count + feats
    pad = -(-vec_count // 8) * 8
    pair_count = vec_count * (vec_count - 1) // 2
    pair_pad = -(-pair_count // LANES) * LANES
    return pl.pallas_call(
        functools.partial(top_kernel, vec_count, pad),
        out_shape=(
            jax.ShapeDtypeStruct((small_count, batch, width), bf16),
            jax.ShapeDtypeStruct((feats, bag_span, width), bf16),
        ),
        in_specs=[whole(pltpu.SMEM)] * 2 + [whole(pltpu.VMEM)] * 7,
        out_specs=(whole(pltpu.VMEM), whole(pltpu.VMEM)),
        scratch_shapes=[
            pltpu.VMEM((batch * pad, width), f32),
            pltpu.VMEM((batch * pad, LANES), f32),
            pltpu.VMEM((batch, pair_pad), bf16),
            pltpu.VMEM((batch, pair_pad), f32),
        ],
        compiler_params=pltpu.CompilerParams(vmem_limit_bytes=VMEM_LIMIT),
        name="top",
    )(
        index, sizes, dense, labels[None, :], small, large, w_first,
        bias[None, :], wout[None, :],
    )


def greet_all():
    copies, groups = lax.axis_size("rep"), lax.axis_size("shard")
    devices = copies * groups
    index = lax.axis_index("rep") * groups + lax.axis_index("shard")
    barrier = pltpu.get_barrier_semaphore()

    def greet(k, c):
        other = lax.rem(index + k, devices)
        pl.semaphore_signal(
            barrier, inc=1, device_id={"rep": other // groups, "shard": lax.rem(other, groups)},
            device_id_type=pl.DeviceIdType.MESH,
        )
        return c

    lax.fori_loop(1, devices, greet, 0)
    pl.semaphore_wait(barrier, devices - 1)


def remote(src, dst, send, recv, rep, shard):
    return pltpu.make_async_remote_copy(
        src_ref=src, dst_ref=dst, send_sem=send, recv_sem=recv,
        device_id={"rep": rep, "shard": shard}, device_id_type=pl.DeviceIdType.MESH,
    )


def forward_kernel(
    pooled_ref, ids_ref, own_ids_ref, tables_ref, large_out, ids_out, small_out,
    send, recv, id_send, id_recv, own, tables,
):
    copies, groups = lax.axis_size("rep"), lax.axis_size("shard")
    devices = copies * groups
    rep, me = lax.axis_index("rep"), lax.axis_index("shard")
    index = rep * groups + me

    def block(k):
        to = lax.rem(me + k, groups)
        return remote(pooled_ref.at[to], large_out.at[me], send.at[k], recv.at[k], rep, to)

    def ids(k):
        to = lax.rem(index + k, devices)
        return remote(
            ids_ref.at[to], ids_out.at[index], id_send.at[k], id_recv.at[k],
            to // groups, lax.rem(to, groups),
        )

    def block_in(k):
        at = lax.rem(me + groups - k, groups)
        return remote(pooled_ref.at[at], large_out.at[at], send.at[k], recv.at[k], rep, at)

    def ids_in(k):
        at = lax.rem(index + devices - k, devices)
        return remote(
            ids_ref.at[at], ids_out.at[at], id_send.at[k], id_recv.at[k],
            at // groups, lax.rem(at, groups),
        )

    def run(low, high, act):
        def body(k, c):
            act(k)
            return c

        lax.fori_loop(low, high, body, 0)

    fetch = pltpu.make_async_copy(tables_ref, tables, own.at[2])
    fetch.start()
    greet_all()
    run(1, groups, lambda k: block(k).start())
    run(1, devices, lambda k: ids(k).start())
    mine = pltpu.make_async_copy(pooled_ref.at[me], large_out.at[me], own.at[0])
    mine_ids = pltpu.make_async_copy(ids_ref.at[index], ids_out.at[index], own.at[1])
    mine.start()
    mine_ids.start()
    batch, small_count = own_ids_ref.shape
    rows = iota((batch, tables_ref.shape[1]), 1)
    fetch.wait()
    for t in range(small_count):
        hot = (own_ids_ref[:, t : t + 1] == rows).astype(f32).astype(bf16)
        small_out[t] = jnp.dot(hot, tables[t], preferred_element_type=f32).astype(bf16)
    mine.wait()
    mine_ids.wait()
    run(1, groups, lambda k: block_in(k).wait_recv())
    run(1, devices, lambda k: ids_in(k).wait_recv())
    run(1, groups, lambda k: block(k).wait_send())
    run(1, devices, lambda k: ids(k).wait_send())


def forward(pooled, ids, own_ids, tables):
    groups, devices = pooled.shape[0], ids.shape[0]
    return pl.pallas_call(
        forward_kernel,
        out_shape=(
            jax.ShapeDtypeStruct(pooled.shape, pooled.dtype),
            jax.ShapeDtypeStruct(ids.shape, ids.dtype),
            jax.ShapeDtypeStruct(
                (tables.shape[0], own_ids.shape[0], tables.shape[2]), tables.dtype
            ),
        ),
        in_specs=[whole(pltpu.VMEM)] * 3 + [whole(pl.ANY)],
        out_specs=(whole(pltpu.VMEM),) * 3,
        scratch_shapes=[pltpu.SemaphoreType.DMA((groups,))] * 2
        + [pltpu.SemaphoreType.DMA((devices,))] * 2
        + [pltpu.SemaphoreType.DMA((3,)), pltpu.VMEM(tables.shape, tables.dtype)],
        compiler_params=pltpu.CompilerParams(
            collective_id=0, has_side_effects=True, vmem_limit_bytes=VMEM_LIMIT
        ),
        name="forward",
    )(pooled, ids, own_ids, tables)


def fold_kernel(fold_ref, out_ref, send, recv, far_send, far_recv, own):
    copies, groups = lax.axis_size("rep"), lax.axis_size("shard")
    rep, me = lax.axis_index("rep"), lax.axis_index("shard")
    other = 1 - rep

    def out_block(k):
        to = lax.rem(me + k, groups)
        return remote(
            fold_ref.at[to], out_ref.at[rep * groups + me], send.at[k], recv.at[k], rep, to
        )

    def in_block(k):
        at = lax.rem(me + groups - k, groups)
        return remote(
            fold_ref.at[at], out_ref.at[rep * groups + at], send.at[k], recv.at[k], rep, at
        )

    def far_out(k):
        slot = out_ref.at[rep * groups + lax.rem(me + groups - k, groups)]
        return remote(slot, slot, far_send.at[k], far_recv.at[k], other, me)

    def far_in(k):
        slot = out_ref.at[other * groups + lax.rem(me + groups - k, groups)]
        return remote(slot, slot, far_send.at[k], far_recv.at[k], other, me)

    own_far = remote(
        fold_ref.at[me], out_ref.at[rep * groups + me], far_send.at[0], far_recv.at[0], other, me
    )

    def run(act):
        def body(k, c):
            act(k)
            return c

        lax.fori_loop(1, groups, body, 0)

    greet_all()
    run(lambda k: out_block(k).start())
    own_far.start()
    mine = pltpu.make_async_copy(fold_ref.at[me], out_ref.at[rep * groups + me], own.at[0])
    mine.start()

    def pass_on(k):
        in_block(k).wait_recv()
        far_out(k).start()

    run(pass_on)
    mine.wait()
    far_in(0).wait_recv()
    run(lambda k: far_in(k).wait_recv())
    own_far.wait_send()
    run(lambda k: far_out(k).wait_send())
    run(lambda k: out_block(k).wait_send())


def fold_exchange(fold, copies):
    groups = fold.shape[0]
    return pl.pallas_call(
        fold_kernel,
        out_shape=jax.ShapeDtypeStruct((copies * groups,) + fold.shape[1:], fold.dtype),
        in_specs=[whole(pltpu.VMEM)],
        out_specs=whole(pltpu.VMEM),
        scratch_shapes=[pltpu.SemaphoreType.DMA((groups,))] * 4 + [pltpu.SemaphoreType.DMA((1,))],
        compiler_params=pltpu.CompilerParams(
            collective_id=1, has_side_effects=True, vmem_limit_bytes=VMEM_LIMIT
        ),
        cost_estimate=pl.CostEstimate(
            flops=400 * fold.size * LANES, bytes_accessed=4 * fold.size, transcendentals=0
        ),
        name="fold_exchange",
    )(fold)


def spread_kernel(own_ref, out_ref, send_z, send_1, send_2, send_core, recv, local):
    groups = lax.axis_size("shard")
    ring = groups // 4
    rep, member = lax.axis_index("rep"), lax.axis_index("shard")
    z, y, core = member // 4, lax.rem(member, 4) // 2, lax.rem(member, 2)

    def shard_of(z_at, y_at, core_at):
        return z_at * 4 + y_at * 2 + core_at

    def send(h, src, rep_at, z_at, y_at, sem, to_rep, to_z, to_y, to_core):
        slot = rep_at * groups + shard_of(z_at, y_at, core)
        source = out_ref.at[slot, h] if src is None else src
        return remote(
            source, out_ref.at[slot, h], sem, recv.at[h, slot],
            to_rep, shard_of(to_z, to_y, to_core),
        )

    def arrived(h, rep_at, z_at, y_at, core_at):
        slot = rep_at * groups + shard_of(z_at, y_at, core_at)
        place = out_ref.at[slot, h]
        remote(place, place, local.at[1], recv.at[h, slot], rep, member).wait_recv()

    greet_all()
    pending = []

    def go(copy):
        copy.start()
        pending.append(copy)

    def second(h, k, src, rep_at, z_at, y_at):
        hop = (rep, z, 1 - y, core) if h == 0 else (1 - rep, z, y, core)
        go(send(h, src, rep_at, z_at, y_at, send_1.at[h, k], *hop))

    def third(h, k, src, rep_at, z_at, y_at):
        hop = (1 - rep, z, y, core) if h == 0 else (rep, z, 1 - y, core)
        go(send(h, src, rep_at, z_at, y_at, send_2.at[h, k], *hop))

    def last(h, k, src, rep_at, z_at, y_at):
        go(send(h, src, rep_at, z_at, y_at, send_core.at[h, k], rep, z, y, 1 - core))

    for k in range(1, ring):
        for h in range(2):
            go(send(h, own_ref.at[h], rep, z, y, send_z.at[h, k], rep, lax.rem(z + k, ring), y, core))
    for h in range(2):
        src = own_ref.at[h]
        second(h, 0, src, rep, z, y)
        third(h, 0, src, rep, z, y)
        last(h, 0, src, rep, z, y)
    mine = pltpu.make_async_copy(
        own_ref, out_ref.at[rep * groups + member], local.at[0]
    )
    mine.start()
    for k in range(1, ring):
        z_at = lax.rem(z + ring - k, ring)
        for h in range(2):
            arrived(h, rep, z_at, y, core)
            second(h, k, None, rep, z_at, y)
            third(h, k, None, rep, z_at, y)
            last(h, k, None, rep, z_at, y)
    for k in range(ring):
        z_at = lax.rem(z + ring - k, ring)
        for h in range(2):
            where = (rep, z_at, 1 - y) if h == 0 else (1 - rep, z_at, y)
            arrived(h, *where, core)
            third(h, ring + k, None, *where)
            last(h, ring + k, None, *where)
    for k in range(2 * ring):
        z_at = lax.rem(z + ring - k % ring, ring)
        for h in range(2):
            if h == 0:
                where = (1 - rep, z_at, y if k < ring else 1 - y)
            else:
                where = (rep if k < ring else 1 - rep, z_at, 1 - y)
            arrived(h, *where, core)
            last(h, 2 * ring + k, None, *where)
    for r in range(2):
        for k in range(ring):
            for y_at in range(2):
                for h in range(2):
                    arrived(h, r, k, y_at, 1 - core)
    mine.wait()
    for copy in pending:
        copy.wait_send()


def spread_all(own, copies, groups):
    rows, width = own.shape
    ring = groups // 4
    devices = copies * groups
    out = pl.pallas_call(
        spread_kernel,
        out_shape=jax.ShapeDtypeStruct((devices, 2, rows // 2, width), own.dtype),
        in_specs=[whole(pltpu.VMEM)],
        out_specs=whole(pltpu.VMEM),
        scratch_shapes=[
            pltpu.SemaphoreType.DMA((2, ring)),
            pltpu.SemaphoreType.DMA((2, ring)),
            pltpu.SemaphoreType.DMA((2, 2 * ring)),
            pltpu.SemaphoreType.DMA((2, 4 * ring)),
            pltpu.SemaphoreType.DMA((2, devices)),
            pltpu.SemaphoreType.DMA((2,)),
        ],
        compiler_params=pltpu.CompilerParams(
            collective_id=2, has_side_effects=True, vmem_limit_bytes=VMEM_LIMIT
        ),
        name="spread_all",
    )(own.reshape(2, rows // 2, width))
    return out.reshape(devices * rows, width)


def shards(
    dense, small_ids, labels, small_tables, large_tables, batch_sizes, bag_ends,
    owner_row_index, w_first, b_first, w_out,
):
    groups = lax.axis_size("shard")
    copies = lax.axis_size("rep")
    devices = groups * copies
    first = lax.axis_index("rep") * groups
    index = first + lax.axis_index("shard")
    small_count, small_rows, width = small_tables.shape
    per_table = devices // small_count
    ends, rows, table = bag_ends[0], owner_row_index[0], large_tables[0]

    pooled, sent_ids, own_ids = pool(
        first[None], groups, rows, ends, table, jnp.transpose(small_ids), devices
    )
    large, all_ids, small = forward(pooled, sent_ids, own_ids, small_tables)
    small_grads, fold = top(
        index[None], batch_sizes, dense, labels, small, large, w_first, b_first, w_out
    )
    fold_all = fold_exchange(fold, copies)
    sent = jnp.repeat(small_grads, per_table, axis=0)
    sent, fold_all = lax.optimization_barrier((sent, fold_all))
    arrived = lax.all_to_all(sent, ("rep", "shard"), split_axis=0, concat_axis=0, tiled=True)
    large_new = scatter(rows, ends, fold_all, table)
    part_rows = small_count * small_rows // devices
    flat = small_tables.reshape(small_count * small_rows, width)
    own = lax.dynamic_slice_in_dim(flat, index * part_rows, part_rows, 0)
    first_row = (lax.rem(index, per_table) * part_rows)[None].astype(jnp.int32)
    updated = small_update(first_row, all_ids[:, 0], arrived, own)
    small_new = spread_all(updated, copies, groups).reshape(small_count, small_rows, width)
    return small_new, large_new[None]


def solution(mesh):
    both = ("rep", "shard")
    placed = (
        P(both, None), P(both, None), P(both), P(), P("shard", None, None), P(),
        P("shard", None, None), P("shard", None, None), P(), P(), P(),
    )
    return jax.shard_map(
        shards, mesh=mesh, in_specs=placed, out_specs=(P(), P("shard", None, None)), check_vma=False
    )
```
